256 devices in a mesh: root: 8 (over z), virt: 16 (over x, y), occ: 2 (over core).
Axes of the slice: x: 4, y: 4, z: 8, core: 2. Of those that a mesh axis runs over, the one named last changes fastest.
Arguments:
- trial_singles: bfloat16 [16, 96], P('root'), may hold values from -6 to 6
- trial_doubles: bfloat16 [16, 480, 9216], P('root', 'virt', 'occ'), may hold values from -6 to 6
- occ_fock: bfloat16 [96, 96], replicated, may hold values from -0.625 to 0.625
- virt_fock: bfloat16 [480, 480], replicated, may hold values from -0.25 to 0.25
- w_ovoo: bfloat16 [96, 480, 9216], P('occ', 'virt', 'root'), may hold values from -0.625 to 0.625
- w_ooov: bfloat16 [96, 480, 9216], P('occ', 'virt', 'root'), may hold values from -0.0029296875 to 0.0029296875
- converged: int32 [16], replicated, may hold values from 0 to 1, as said below
Outputs:
- sigma_doubles: bfloat16 [16, 480, 9216], P('root', 'virt', 'occ')
- sigma_singles: float32 [16, 96], P('root')
- subspace: float32 [16, 16], P('root')
The draws below stay inside these ranges and needn't reach their ends.
Inputs may be any that keep to these rules, and one draw needn't show every extreme that they name: `converged`: exactly 8 roots are active (0). In every draw at least one aligned block of 2 roots has all its roots active; other blocks may have none.
All inputs are finite; a program needn't handle non-finite values.
Results may differ from the reference program's by a relative error of at most 0.0044.
Values may be sent and summed in bfloat16 or wider, within the bound.
No kernel may reach another device: no remote copies, remote signals or barrier semaphores. Data moves between devices by JAX's collectives and lax.ppermute only.
A program may use at most 256 MiB of HBM per device.

```python
import math
import jax
import jax.numpy as jnp
from jax import lax

O = 96
V = 480
ROOTS_DEV = 2
ROOTS = 16


def draw_converged(key, part):
    groups = ROOTS // ROOTS_DEV
    level = jax.random.randint(jax.random.fold_in(key, 11), (groups,), 0, 4)
    chosen = jax.random.randint(jax.random.fold_in(key, 13), (), 0, groups)
    level = level.at[chosen].set(4)
    noise = jax.random.randint(jax.random.fold_in(key, 12), (ROOTS,), 0, ROOTS)
    positions = jnp.arange(ROOTS, dtype=jnp.int32)
    group_of = positions // ROOTS_DEV
    score = (level[group_of] * ROOTS + noise) * ROOTS + positions
    ranking = jnp.argsort(jnp.argsort(-score))
    return (ranking >= ROOTS // 2).astype(jnp.int32)


def levels(rng, dims, shards, low, high):
    def one(position, parts):
        draws = jax.random.uniform(jax.random.fold_in(jax.random.fold_in(rng, 6), position), (parts,), jnp.float32, low / len(shards), high / len(shards))
        return jnp.repeat(jnp.exp(draws), dims[position] // parts).reshape((-1,) + (1,) * (len(dims) - position - 1))

    gain = one(*shards[0])
    for cut in shards[1:]:
        gain = gain * one(*cut)
    return gain


def scatter_about(stream_key, extent, width, limit, cuts=(), kind=jnp.bfloat16):
    loudness = levels(stream_key, extent, cuts, -0.22, 0.18) if cuts else 1.0
    values = jax.random.normal(stream_key, extent, jnp.float32) * width * loudness
    return jnp.minimum(jnp.maximum(values, -limit), limit).astype(kind)


def setup_inputs(seed: int = 0) -> dict:
    streams_of = jax.random.split(jax.random.key(seed), 8)
    trial_singles = scatter_about(streams_of[0], (ROOTS, O), 1.0, 6.0, ((0, 8),))
    trial_doubles = scatter_about(streams_of[1], (ROOTS, V, O * O), 1.0, 6.0, ((0, 8), (1, 16), (2, 2)))
    occ_fock = scatter_about(streams_of[2], (O, O), O ** -0.5, 0.625)
    virt_fock = scatter_about(streams_of[3], (V, V), V ** -0.5, 0.25)
    w_ovoo = scatter_about(streams_of[4], (O, V, O * O), O ** -0.5, 0.625, ((0, 2), (1, 16), (2, 8)))
    w_ooov = scatter_about(streams_of[5], (O, V, O * O), (O * O * V) ** -0.5, 0.0029296875, ((0, 2), (1, 16), (2, 8)))
    converged = draw_converged(jax.random.fold_in(streams_of[7], 71), 0)
    return {"trial_singles": trial_singles, "trial_doubles": trial_doubles, "occ_fock": occ_fock, "virt_fock": virt_fock, "w_ovoo": w_ovoo, "w_ooov": w_ooov, "converged": converged}


def reference(trial_singles, trial_doubles, occ_fock, virt_fock, w_ovoo, w_ooov, converged):
    active = (1 - converged).astype(jnp.float32)
    outer_flat = w_ovoo.reshape(O, V * O * O)
    inner_flat = w_ooov.reshape(O, V * O * O)
    occ_wide = occ_fock.astype(jnp.float32)

    def per_root(bundle):
        single_row, double_block, weight_now = bundle
        outer_term = (-jnp.dot(single_row[None, :], outer_flat, preferred_element_type=jnp.float32)).reshape(V, O, O)
        vv_term = jnp.dot(virt_fock, double_block, preferred_element_type=jnp.float32).astype(jnp.bfloat16).reshape(V, O, O)
        block_wide = double_block.reshape(V, O, O).astype(jnp.float32)
        first_term = jnp.einsum('ki,akj->aij', occ_wide, block_wide)
        second_term = jnp.einsum('kj,aik->aij', occ_wide, block_wide)
        summed = weight_now * (vv_term.astype(jnp.float32) + outer_term - first_term - second_term)
        coupling = jnp.dot(inner_flat, double_block.reshape(V * O * O), preferred_element_type=jnp.float32)
        return (summed.reshape(V, O * O).astype(jnp.bfloat16), coupling)
    sigma_doubles, coupling = lax.map(per_root, (trial_singles, trial_doubles, active))
    singles_fock = jnp.dot(trial_singles, occ_fock, preferred_element_type=jnp.float32)
    sigma_singles = active[:, None] * (-singles_fock - 0.5 * coupling)
    doubles_part = jnp.dot(trial_doubles.reshape(ROOTS, V * O * O), sigma_doubles.reshape(ROOTS, V * O * O).T, preferred_element_type=jnp.float32)
    singles_part = jnp.dot(trial_singles.astype(jnp.float32), sigma_singles.T, precision=lax.Precision.HIGHEST)
    subspace = doubles_part / math.sqrt(O * O * V) + singles_part / math.sqrt(O)
    return (sigma_doubles, sigma_singles, subspace)
```

```python
import math

import jax
import jax.numpy as jnp
from jax import lax
from jax.experimental import pallas as pl
from jax.experimental.pallas import tpu as pltpu
from jax.sharding import Mesh
from jax.sharding import PartitionSpec as P


VIRT = ("virt_0", "virt_1")
REST = ("virt_0", "virt_1", "occ")
BF = jnp.bfloat16
F32 = jnp.float32
HI = lax.Precision.HIGHEST

Z = 8
NV = 16
OC = 96
VL = 30
VP = 32
BLK = 1152
HALF = 4608
COLS = 640
KH = 48
SPARE = 30
GRP = 384

VMEM = pltpu.VMEM
SMEM = pltpu.SMEM


def iota(shape, dim):
    return lax.broadcasted_iota(jnp.int32, shape, dim)


def dot(a, b, precision=None):
    return jnp.dot(a, b, preferred_element_type=F32, precision=precision)


def dot_nt(a, b, precision=None):
    return lax.dot_general(
        a, b, (((1,), (1,)), ((), ())), preferred_element_type=F32, precision=precision
    )


def call(kernel, outs, places, scratch=(), limit=32, flops=1 << 24, name=None):
    return pl.pallas_call(
        kernel,
        out_shape=outs,
        in_specs=[pl.BlockSpec(memory_space=p) for p in places],
        out_specs=jax.tree.map(lambda _: pl.BlockSpec(memory_space=VMEM), outs),
        scratch_shapes=scratch,
        compiler_params=pltpu.CompilerParams(vmem_limit_bytes=limit << 20),
        cost_estimate=pl.CostEstimate(flops=flops, bytes_accessed=1 << 20, transcendentals=0),
        name=name,
    )


def shape(dims, dtype):
    return jax.ShapeDtypeStruct(dims, dtype)


def other_core(x):
    return lax.ppermute(x, "occ", [(0, 1), (1, 0)])


def z_exchange(x):
    return [x[0]] + [
        lax.ppermute(x[s], "root", [(i, (i + s) % Z) for i in range(Z)]) for s in range(1, Z)
    ]


def prep_kernel(ids, own, recv, t1, zb, xb):
    me, core = ids[0], ids[1]
    rows = iota((2, BLK), 0)
    row = jnp.where(iota((2, OC), 0) == core, t1[...].astype(F32), 0.0)
    row = jnp.sum(row, axis=0, keepdims=True)
    place = (iota((OC, 128), 0) == iota((OC, 128), 1)).astype(F32)
    wide = dot(row, place, HI)
    tail = jnp.concatenate([wide] + [jnp.zeros((1, 128), F32)] * (BLK // 128 - 1), axis=1)
    tail = jnp.where(rows == 0, jnp.broadcast_to(tail, (2, BLK)), 0.0).astype(BF)

    def fill(own_half):
        for h in range(2):
            ref = (lambda c, n: own[own_half, :, c : c + n]) if h == own_half else (
                lambda c, n: recv[:, c : c + n]
            )
            for q in range(4):
                slot = lax.rem(4 * h + q - me + Z, Z)
                zb[slot, 0:VL, :] = ref(BLK * q, BLK)
                zb[slot, VL:VP, :] = tail
            tile = 0
            while tile < 36:
                g, off = divmod(36 * h + tile, 5)
                n = min(5 - off, 36 - tile)
                xb[g, 0:VL, 128 * off : 128 * (off + n)] = ref(128 * tile, 128 * n)
                tile += n

    xb[:, VL:VP, :] = jnp.zeros((NV, VP - VL, COLS), BF)
    xb[14, 0:VL, 256:COLS] = jnp.zeros((VL, COLS - 256), BF)
    xb[15, 0:VL, :] = jnp.zeros((VL, COLS), BF)
    pl.when(core == 0)(lambda: fill(0))
    pl.when(core == 1)(lambda: fill(1))


def oo_kernel(ids, zb, fock, oo, left, stack):
    me = ids[0]
    f = fock[...]
    e3 = (lax.rem(iota((GRP, OC), 0), OC) == iota((GRP, OC), 1)).astype(BF)
    same = iota((GRP, GRP), 0) // OC == iota((GRP, GRP), 1) // OC
    bd = dot_nt(dot(e3, f).astype(BF), e3)
    bd = jnp.where(same, bd, 0.0).astype(BF)
    diag = lax.rem(iota((GRP, GRP), 0), 16) == lax.rem(iota((GRP, GRP), 1), 16)
    for i in range(4):
        e1 = (iota((GRP, OC), 1) == 4 * (iota((GRP, OC), 0) // 16) + i).astype(BF)
        ef = dot_nt(e1, f).astype(BF)
        for s in range(4):
            e2 = (iota((OC, GRP), 0) == 4 * (iota((OC, GRP), 1) // 16) + (i - s) % 4).astype(BF)
            m = jnp.where(diag, dot(ef, e2), 0.0).astype(BF)
            left[i, :, GRP * s : GRP * (s + 1)] = m
    segment = iota((GRP, GRP), 1) // OC
    for b in range(2):
        for r in range(Z):
            slot = lax.rem(r - me + Z, Z)
            for q in range(3):
                g = 3 * r + q
                stack[16 * g : 16 * (g + 1), :] = zb[
                    slot, 16 * b : 16 * (b + 1), GRP * q : GRP * (q + 1)
                ]
        base = stack[0:GRP, :]
        wide = base.astype(F32)
        for s in range(1, 4):
            stack[GRP * s : GRP * (s + 1), :] = pltpu.roll(wide, OC * s, 1).astype(BF)
        total = dot(base, bd)
        for i in range(4):
            total += jnp.where(segment == i, dot(left[i], stack[...]), 0.0)
        for r in range(Z):
            for q in range(3):
                g = 3 * r + q
                oo[r, 16 * b : 16 * (b + 1), GRP * q : GRP * (q + 1)] = total[
                    16 * g : 16 * (g + 1), :
                ]


def mm_kernel(fock, x, out):
    n = NV * VP
    count = NV * VL
    row = iota((n, count), 0)
    pick = (VL * (row // VP) + lax.rem(row, VP) == iota((n, count), 1)) & (lax.rem(row, VP) < VL)
    pick = pick.astype(BF)
    padded = dot_nt(dot(pick, fock[...]).astype(BF), pick).astype(BF)
    y = dot(padded, x[...].reshape(n, COLS)).astype(BF)
    out[...] = y.reshape(NV, VP, COLS)


def gather_kernel(ids, *refs):
    me = ids[0]
    out = refs[Z]
    for s in range(Z):
        out[lax.rem(me - s + Z, Z)] = refs[s][...]


def singles_of(ref):
    mask = iota((16, 128), 0) == SPARE - 16
    rows = []
    for r in range(Z):
        x = ref[r, 16:32, 0:128].astype(F32)
        rows.append(jnp.sum(jnp.where(mask, x, 0.0), axis=0, keepdims=True))
    return jnp.concatenate(rows, axis=0)


def load_pad(w, pad):
    pad[:, 14:16, :] = jnp.zeros((KH, 2, BLK), BF)
    pad[:, 0:14, :] = w[:, 16:30, :]


def outer_kernel(ids, mine, theirs, w, out_mine, out_theirs, pad):
    core = ids[1]
    load_pad(w, pad)
    t1 = jnp.concatenate([singles_of(mine), singles_of(theirs)], axis=0).astype(BF)
    k = KH * 16
    e1 = (iota((256, 16), 0) // 16 == iota((256, 16), 1)).astype(BF)
    e2 = (iota((128, k), 0) == KH * core + iota((128, k), 1) // 16).astype(BF)
    spread = dot(dot(e1, t1).astype(BF), e2)
    diag = lax.rem(iota((256, k), 0), 16) == lax.rem(iota((256, k), 1), 16)
    spread = jnp.where(diag, -spread, 0.0).astype(BF)
    for b in range(2):
        rhs = (w[:, 0:16, :] if b == 0 else pad[...]).reshape(k, BLK)
        y = dot(spread, rhs).astype(BF)
        for n in range(Z):
            out_mine[n, 16 * b : 16 * (b + 1), :] = y[16 * n : 16 * (n + 1), :]
            out_theirs[n, 16 * b : 16 * (b + 1), :] = y[128 + 16 * n : 128 + 16 * (n + 1), :]


def add_kernel(ids, a, b, out):
    me = ids[0]
    for s in range(Z):
        r = lax.rem(me + s, Z)
        out[s] = (a[r].astype(F32) + b[r].astype(F32)).astype(BF)


def folded(g, b):
    rows, cols = g.shape
    a, c = lax.rem(iota(g.shape, 0), 16), lax.rem(iota(g.shape, 1), 16)
    g = jnp.where((a == c) & (a < (16 if b == 0 else VL - 16)), g, 0.0)
    left = (iota((rows // 16, rows), 1) // 16 == iota((rows // 16, rows), 0)).astype(F32)
    right = (iota((cols, cols // 16), 0) // 16 == iota((cols, cols // 16), 1)).astype(F32)
    return dot(dot(left, g, HI), right, HI)


def coupling_kernel(mine, theirs, w, out, pad):
    load_pad(w, pad)
    k = KH * 16
    for j, t in enumerate((mine, theirs)):
        total = jnp.zeros((Z, KH), F32)
        for b in range(2):
            rhs = (w[:, 0:16, :] if b == 0 else pad[...]).reshape(k, BLK)
            lhs = t[:, 16 * b : 16 * (b + 1), :].reshape(128, BLK)
            total += folded(dot_nt(lhs, rhs), b)
        out[j] = total


def x_kernel(ids, vv, oo, x, xb):
    me = ids[0]
    for r in range(Z):
        slot = lax.rem(r - me + Z, Z)
        tile = 0
        while tile < 9:
            g, off = divmod(9 * r + tile, 5)
            n = min(5 - off, 9 - tile)
            lo, hi = 128 * tile, 128 * (tile + n)
            v = vv[g, :, 128 * off : 128 * (off + n)].astype(F32) - oo[r, :, lo:hi]
            x[r, :, lo:hi] = v
            xb[slot, :, lo:hi] = v.astype(BF)
            tile += n


def s_kernel(ids, mine, theirs, ov, coupling, *refs):
    me, core = ids[0], ids[1]
    out, t1_out, y = refs[Z], refs[Z + 1], refs[Z + 2]
    for s in range(Z):
        n = lax.rem(me - s + Z, Z)
        back = lax.rem(Z - s, Z)
        y[n] = (refs[s][...].astype(F32) + ov[back].astype(F32)).astype(BF)
    t1_mine, t1_theirs = singles_of(mine), singles_of(theirs)
    doubles = [jnp.zeros((Z, Z), F32) for _ in range(2)]
    for b in range(2):
        rhs = y[:, 16 * b : 16 * (b + 1), :].reshape(128, BLK)
        for j, t in enumerate((mine, theirs)):
            lhs = t[:, 16 * b : 16 * (b + 1), :].reshape(128, BLK)
            doubles[j] += folded(dot_nt(lhs, rhs), b)
    half = (iota((128, KH), 0) == KH * core + iota((128, KH), 1)).astype(F32)
    place_c = (iota((KH, 128), 1) == KH * core + iota((KH, 128), 0)).astype(F32)

    def place_n(parity):
        return (iota((Z, 128), 1) == OC + 2 * iota((Z, 128), 0) + parity).astype(F32)

    own_n, far_n = place_n(core), place_n(1 - core)
    scale_d = 1.0 / math.sqrt(OC * OC * NV * VL)
    scale_s = -0.5 / math.sqrt(OC)
    out[...] = jnp.zeros((Z, 8, 128), F32)
    t1_out[...] = jnp.zeros((16, 128), F32)
    for j, t1 in enumerate((t1_mine, t1_theirs)):
        t1_half = dot(t1, half, HI)
        row = dot(coupling[j], place_c, HI)
        row += dot(doubles[j] * scale_d + dot_nt(t1_half, coupling[0], HI) * scale_s, own_n, HI)
        row += dot(dot_nt(t1_half, coupling[1], HI) * scale_s, far_n, HI)
        p = core if j == 0 else 1 - core
        for r in range(Z):
            out[r, pl.ds(p, 1), :] = row[r : r + 1, :]
            t1_out[pl.ds(2 * r + p, 1), :] = t1[r : r + 1, :]


def sum_kernel(x, out):
    out[...] = jnp.broadcast_to(jnp.sum(x[...], axis=0, keepdims=True), out.shape)


def final_kernel(ids, conv, active, x, t1, fock, singles, subspace):
    me = ids[0]
    total = jnp.sum(x[...], axis=0)
    mine = jnp.concatenate([t1[pl.ds(2 * me, 1), :], t1[pl.ds(2 * me + 1, 1), :]], axis=0)[:, 0:OC]
    all_fock = dot(t1[:, 0:OC].astype(BF), fock[...])
    own_fock = dot(mine.astype(BF), fock[...])
    a0 = (1 - conv[2 * me]).astype(F32)
    a1 = (1 - conv[2 * me + 1]).astype(F32)
    own_active = jnp.where(iota((2, OC), 0) == 0, a0, a1)
    singles[...] = own_active * (-own_fock - 0.5 * total[0:2, 0:OC])
    part = total[0:2, OC : OC + 2 * Z] - dot_nt(mine, all_fock, HI) * (1.0 / math.sqrt(OC))
    subspace[...] = part * active[...]


def out_kernel(ids, conv, x, *refs):
    me, core = ids[0], ids[1]
    out, ov = refs[Z], refs[Z + 1]
    a = (1 - conv[2 * me + core]).astype(F32)
    for s in range(Z):
        ov[lax.rem(me - s + Z, Z)] = refs[s][...]
    for r in range(Z):
        h, q = divmod(r, 4)
        v = a * (x[r, 0:VL, :] + ov[r, 0:VL, :].astype(F32))
        out[h, :, BLK * q : BLK * (q + 1)] = v.astype(BF)


def join_kernel(ids, own, recv, out):
    core = ids[1]
    out[pl.ds(core, 1)] = own[pl.ds(core, 1)]
    out[pl.ds(1 - core, 1)] = recv[...].reshape(1, VL, HALF)


def local(trial_singles, trial_doubles, occ_fock, virt_fock, w_ovoo, w_ooov, converged):
    core = lax.axis_index("occ")
    ids = jnp.stack([lax.axis_index("root"), core]).astype(jnp.int32)
    active = (1 - converged).astype(F32)[None, :]

    swapped = other_core(lax.dynamic_index_in_dim(trial_doubles, 1 - core, 0, keepdims=False))
    zb, xb = call(
        prep_kernel,
        (shape((Z, VP, BLK), BF), shape((NV, VP, COLS), BF)),
        [SMEM, VMEM, VMEM, VMEM],
        name="prep",
    )(ids, trial_doubles, swapped, trial_singles)

    gathered = lax.all_to_all(xb, VIRT, split_axis=0, concat_axis=0, tiled=True)
    blocks = z_exchange(zb)
    oo = call(
        oo_kernel,
        shape((Z, VP, BLK), F32),
        [SMEM, VMEM, VMEM],
        [VMEM((4, GRP, 4 * GRP), BF), VMEM((4 * GRP, GRP), BF)],
        flops=4 << 30,
        name="oo",
    )(ids, zb, occ_fock)
    product = call(
        mm_kernel, shape((NV, VP, COLS), BF), [VMEM, VMEM], flops=1 << 29, name="mm"
    )(virt_fock, gathered)
    vv = lax.all_to_all(product, VIRT, split_axis=0, concat_axis=0, tiled=True)

    mine = call(gather_kernel, shape((Z, VP, BLK), BF), [SMEM] + [VMEM] * Z, name="gather")(
        ids, *blocks
    )
    theirs = other_core(mine)
    outer_mine, outer_theirs = call(
        outer_kernel,
        (shape((Z, VP, BLK), BF), shape((Z, VP, BLK), BF)),
        [SMEM, VMEM, VMEM, VMEM],
        [VMEM((KH, 16, BLK), BF)],
        flops=1 << 30,
        name="outer",
    )(ids, mine, theirs, w_ovoo)
    ov = call(add_kernel, shape((Z, VP, BLK), BF), [SMEM, VMEM, VMEM], name="add")(
        ids, outer_mine, other_core(outer_theirs)
    )
    ov_owned = z_exchange(ov)
    coupling = call(
        coupling_kernel,
        shape((2, Z, KH), F32),
        [VMEM, VMEM, VMEM],
        [VMEM((KH, 16, BLK), BF)],
        flops=1 << 30,
        name="coupling",
    )(mine, theirs, w_ooov)

    x, xr = call(
        x_kernel,
        (shape((Z, VP, BLK), F32), shape((Z, VP, BLK), BF)),
        [SMEM, VMEM, VMEM],
        name="x",
    )(ids, vv, oo)
    x_blocks = z_exchange(xr)
    message, t1 = call(
        s_kernel,
        (shape((Z, 8, 128), F32), shape((16, 128), F32)),
        [SMEM] + [VMEM] * (Z + 4),
        [VMEM((Z, VP, BLK), BF)],
        name="s",
    )(ids, mine, theirs, ov, coupling, *x_blocks)
    arrived = lax.all_to_all(message, "root", split_axis=0, concat_axis=0, tiled=True)
    copies = call(sum_kernel, shape((32, 8, 128), F32), [VMEM], name="sum")(arrived)
    arrived = lax.all_to_all(copies, REST, split_axis=0, concat_axis=0, tiled=True)
    sigma_singles, subspace = call(
        final_kernel,
        (shape((2, OC), F32), shape((2, 2 * Z), F32)),
        [SMEM, SMEM, VMEM, VMEM, VMEM, VMEM],
        name="final",
    )(ids, converged, active, arrived, t1, occ_fock)

    halves = call(
        out_kernel,
        shape((2, VL, HALF), BF),
        [SMEM, SMEM] + [VMEM] * (Z + 1),
        [VMEM((Z, VP, BLK), BF)],
        name="out",
    )(ids, converged, x, *ov_owned)
    recv = other_core(lax.dynamic_index_in_dim(halves, 1 - core, 0, keepdims=False))
    sigma_doubles = call(join_kernel, shape((2, VL, HALF), BF), [SMEM, VMEM, VMEM], name="join")(
        ids, halves, recv
    )
    return (sigma_doubles, sigma_singles, subspace)


def solution(mesh):
    torus = Mesh(
        mesh.devices.reshape(mesh.shape["root"], 4, 4, mesh.shape["occ"]),
        ("root", "virt_0", "virt_1", "occ"),
    )
    return jax.shard_map(
        local,
        mesh=torus,
        in_specs=(
            P("root", None),
            P("root", VIRT, "occ"),
            P(),
            P(),
            P("occ", VIRT, "root"),
            P("occ", VIRT, "root"),
            P(),
        ),
        out_specs=(P("root", VIRT, "occ"), P("root", None), P("root", None)),
        check_vma=False,
    )
```

```python
import math

import jax
import jax.numpy as jnp
from jax import lax
from jax.experimental import pallas as pl
from jax.experimental.pallas import tpu as pltpu
from jax.sharding import Mesh
from jax.sharding import PartitionSpec as P


VIRT = ("virt_0", "virt_1")
REST = ("virt_0", "virt_1", "occ")
BF = jnp.bfloat16
F32 = jnp.float32
HI = lax.Precision.HIGHEST

Z = 8
NV = 16
OC = 96
VL = 30
VP = 32
BLK = 1152
HALF = 4608
COLS = 640
KH = 48
SPARE = 30
GRP = 384

VMEM = pltpu.VMEM
SMEM = pltpu.SMEM


def iota(shape, dim):
    return lax.broadcasted_iota(jnp.int32, shape, dim)


def dot(a, b, precision=None):
    return jnp.dot(a, b, preferred_element_type=F32, precision=precision)


def dot_nt(a, b, precision=None):
    return lax.dot_general(
        a, b, (((1,), (1,)), ((), ())), preferred_element_type=F32, precision=precision
    )


def call(
    kernel,
    outs,
    places,
    scratch=(),
    limit=32,
    flops=1 << 24,
    grid=(),
    out_spec=None,
    name=None,
):
    def spec(p):
        return p if isinstance(p, pl.BlockSpec) else pl.BlockSpec(memory_space=p)

    return pl.pallas_call(
        kernel,
        out_shape=outs,
        grid=grid,
        in_specs=[spec(p) for p in places],
        out_specs=out_spec or jax.tree.map(lambda _: pl.BlockSpec(memory_space=VMEM), outs),
        scratch_shapes=scratch,
        compiler_params=pltpu.CompilerParams(vmem_limit_bytes=limit << 20),
        cost_estimate=pl.CostEstimate(flops=flops, bytes_accessed=1 << 20, transcendentals=0),
        name=name,
    )


def shape(dims, dtype):
    return jax.ShapeDtypeStruct(dims, dtype)


def other_core(x):
    return lax.ppermute(x, "occ", [(0, 1), (1, 0)])


def z_pairs(t):
    return [
        (2 * r + o, 2 * (4 * o + (r + t) % 4) + r // 4) for r in range(Z) for o in range(2)
    ]


def to_blocks(x):
    return [lax.ppermute(x[t], ("root", "occ"), z_pairs(t)) for t in range(4)]


def to_owners(x):
    back = [[(b, a) for a, b in z_pairs(t)] for t in range(4)]
    return [lax.ppermute(x[t], ("root", "occ"), back[t]) for t in range(4)]


def slot_of(q, me):
    return lax.rem(q - me + Z, 4)


def tiles_of(first, count):
    tile, out = 0, []
    while tile < count:
        g, off = divmod(first + tile, 5)
        n = min(5 - off, count - tile)
        out.append((g, 128 * off, 128 * (off + n), 128 * tile, 128 * (tile + n)))
        tile += n
    return out


def prep_kernel(ids, doubles, t1, zb, xb):
    me = ids[0]
    place = (iota((OC, 128), 0) == iota((OC, 128), 1)).astype(F32)
    wide = dot(t1[...].astype(F32), place, HI)
    first = iota((2, 128), 0) == 0
    xb[:, VL:VP, :] = jnp.zeros((NV, VP - VL, COLS), BF)
    xb[14, 0:VL, 256:COLS] = jnp.zeros((VL, COLS - 256), BF)
    xb[15, 0:VL, :] = jnp.zeros((VL, COLS), BF)
    for p in range(2):
        tail = jnp.where(first, jnp.broadcast_to(wide[p : p + 1, :], (2, 128)), 0.0).astype(BF)
        for q in range(4):
            slot = slot_of(q, me)
            zb[slot, p, 0:VL, :] = doubles[p, :, BLK * q : BLK * (q + 1)]
            zb[slot, p, VL:VP, 0:128] = tail
            zb[slot, p, VL:VP, 128:BLK] = jnp.zeros((VP - VL, BLK - 128), BF)
        for g, a, b, lo, hi in tiles_of(36 * p, 36):
            xb[g, 0:VL, a:b] = doubles[p, :, lo:hi]


def oo_kernel(ids, zb, zo, fock, oo, left, own, stack, rolled):
    me, core = ids[0], ids[1]
    f = fock[...]
    rows, depth, half = 96, 768, 192
    e3 = (lax.rem(iota((GRP, OC), 0), OC) == iota((GRP, OC), 1)).astype(BF)
    same = iota((GRP, GRP), 0) // OC == iota((GRP, GRP), 1) // OC
    bd = dot_nt(dot(e3, f).astype(BF), e3)
    bd = jnp.where(same, bd, 0.0).astype(BF)
    col = iota((OC, depth), 1)
    shift = col // half
    group = lax.rem(col, half) // 8
    group = jnp.where(group < 12, group + 12 * core, group - 12 * core)
    diag = lax.rem(iota((rows, depth), 0), 8) == lax.rem(iota((rows, depth), 1), 8)
    for i in range(4):
        mine = 4 * (12 * core + iota((rows, OC), 0) // 8) + i
        ef = dot_nt((iota((rows, OC), 1) == mine).astype(BF), f).astype(BF)
        e2 = (iota((OC, depth), 0) == 4 * group + ((i - shift) & 3)).astype(BF)
        left[rows * i : rows * (i + 1), :] = jnp.where(diag, dot(ef, e2), 0.0).astype(BF)
    lane = iota((rows, 256), 1) & 127
    for p in range(2):
        for b in range(2):
            for h, ref in enumerate((zb, zo)):
                for q in range(4):
                    slot = slot_of(q, me)
                    for u in range(3):
                        at = 12 * h + 3 * q + u
                        piece = ref[
                            slot, p, 16 * b : 16 * (b + 1), GRP * u : GRP * (u + 1)
                        ].astype(F32)
                        stack[0, 8 * at : 8 * (at + 1), :] = piece[0:8, :]
                        stack[1, 8 * at : 8 * (at + 1), :] = piece[8:16, :]
            for c in range(2):
                wide = stack[c]
                rolled[c, 0:half, :] = wide.astype(BF)
                own[rows * c : rows * (c + 1), :] = wide[0:rows, :].astype(BF)
                for s in range(1, 4):
                    rolled[c, half * s : half * (s + 1), :] = pltpu.roll(wide, OC * s, 1).astype(BF)
            second = dot(own[...], bd)
            for tile in range(3):
                lo, hi = 128 * tile, 128 * (tile + 1)
                rhs = jnp.concatenate([rolled[0, :, lo:hi], rolled[1, :, lo:hi]], axis=1)
                y = dot(left[rows * tile : rows * (tile + 2), :], rhs)
                v = jnp.where(lane < 96 - 32 * tile, y[0:rows, :], y[rows:, :])
                for c in range(2):
                    w = v[:, 128 * c : 128 * (c + 1)] + second[rows * c : rows * (c + 1), lo:hi]
                    for g in range(12):
                        q, u = divmod(g, 3)
                        oo[
                            q,
                            p,
                            16 * b + 8 * c : 16 * b + 8 * (c + 1),
                            GRP * u + lo : GRP * u + hi,
                        ] = w[8 * g : 8 * (g + 1), :]


def mm_kernel(fock, x, out):
    n = NV * VP
    count = NV * VL
    row = iota((n, count), 0)
    pick = (VL * (row // VP) + lax.rem(row, VP) == iota((n, count), 1)) & (lax.rem(row, VP) < VL)
    pick = pick.astype(BF)
    padded = dot_nt(dot(pick, fock[...]).astype(BF), pick).astype(BF)
    y = dot(padded, x[...].reshape(n, COLS)).astype(BF)
    out[...] = y.reshape(NV, VP, COLS)


def gather_kernel(ids, *refs):
    me, out = ids[0], refs[4]
    for t in range(4):
        at = 2 * lax.rem(me - t + Z, 4)
        for p in range(2):
            out[at + p] = refs[t][p]


def singles_of(ref):
    mask = iota((16, 128), 0) == SPARE - 16
    rows = []
    for r in range(Z):
        x = ref[r, 16:32, 0:128].astype(F32)
        rows.append(jnp.sum(jnp.where(mask, x, 0.0), axis=0, keepdims=True))
    return jnp.concatenate(rows, axis=0)


def load_pad(w, pad):
    pad[:, 14:16, :] = jnp.zeros((16, 2, BLK), BF)
    pad[:, 0:14, :] = w[:, 16:30, :]


def outer_kernel(ids, mine, theirs, w, out_mine, out_theirs, pad, total, t1s):
    core, step = ids[1], pl.program_id(0)
    load_pad(w, pad)

    @pl.when(step == 0)
    def _():
        t1s[...] = jnp.concatenate([singles_of(mine), singles_of(theirs)], axis=0)

    e1 = (iota((256, 16), 0) // 16 == iota((256, 16), 1)).astype(BF)
    e2 = (iota((128, 256), 0) == KH * core + 16 * step + iota((128, 256), 1) // 16).astype(BF)
    spread = dot(dot(e1, t1s[...].astype(BF)).astype(BF), e2)
    diag = lax.rem(iota((256, 256), 0), 16) == lax.rem(iota((256, 256), 1), 16)
    spread = jnp.where(diag, -spread, 0.0).astype(BF)
    for b in range(2):
        rhs = (w[:, 0:16, :] if b == 0 else pad[...]).reshape(256, BLK)
        y = dot(spread, rhs)

        @pl.when(step == 0)
        def _():
            total[b] = y

        @pl.when(step == 1)
        def _():
            total[b] = total[b] + y

        @pl.when(step == 2)
        def _():
            z = (total[b] + y).astype(BF)
            for n in range(Z):
                out_mine[n, 16 * b : 16 * (b + 1), :] = z[16 * n : 16 * (n + 1), :]
                out_theirs[n, 16 * b : 16 * (b + 1), :] = z[128 + 16 * n : 128 + 16 * (n + 1), :]


def add_kernel(ids, a, b, out):
    me = ids[0]
    for t in range(4):
        at = 2 * lax.rem(me - t + Z, 4)
        for p in range(2):
            out[t, p] = (a[at + p].astype(F32) + b[at + p].astype(F32)).astype(BF)


def folded(g, b):
    rows, cols = g.shape
    a, c = lax.rem(iota(g.shape, 0), 16), lax.rem(iota(g.shape, 1), 16)
    g = jnp.where((a == c) & (a < (16 if b == 0 else VL - 16)), g, 0.0)
    left = (iota((rows // 16, rows), 1) // 16 == iota((rows // 16, rows), 0)).astype(F32)
    right = (iota((cols, cols // 16), 0) // 16 == iota((cols, cols // 16), 1)).astype(F32)
    return dot(dot(left, g, HI), right, HI)


def coupling_kernel(mine, theirs, w, out, pad, t):
    load_pad(w, pad)

    @pl.when(pl.program_id(0) == 0)
    def _():
        for b in range(2):
            for j, ref in enumerate((mine, theirs)):
                t[b, 128 * j : 128 * (j + 1), :] = ref[:, 16 * b : 16 * (b + 1), :].reshape(
                    128, BLK
                )

    total = jnp.zeros((16, 16), F32)
    for b in range(2):
        lhs = (w[:, 0:16, :] if b == 0 else pad[...]).reshape(256, BLK)
        total += folded(dot_nt(lhs, t[b]), b)
    out[...] = total


def x_kernel(ids, vv, oo, x, xb):
    me = ids[0]
    for p in range(2):
        for q in range(4):
            slot = slot_of(q, me)
            for g, a, b, lo, hi in tiles_of(36 * p + 9 * q, 9):
                v = vv[g, :, a:b].astype(F32) - oo[q, p, :, lo:hi]
                x[q, p, :, lo:hi] = v
                xb[slot, p, :, lo:hi] = v.astype(BF)


def s_kernel(ids, mine, theirs, ov, coupling, *refs):
    me, core = ids[0], ids[1]
    out, t1_out, y = refs[4], refs[5], refs[6]
    for t in range(4):
        at = 2 * lax.rem(me - t + Z, 4)
        for p in range(2):
            y[at + p] = (refs[t][p].astype(F32) + ov[t, p].astype(F32)).astype(BF)
    doubles = [jnp.zeros((Z, Z), F32) for _ in range(2)]
    for b in range(2):
        rhs = y[:, 16 * b : 16 * (b + 1), :].reshape(128, BLK)
        for j, ref in enumerate((mine, theirs)):
            lhs = ref[:, 16 * b : 16 * (b + 1), :].reshape(128, BLK)
            doubles[j] += folded(dot_nt(lhs, rhs), b)
    half = (iota((128, KH), 0) == KH * core + iota((128, KH), 1)).astype(F32)
    place_c = (iota((KH, 128), 1) == KH * core + iota((KH, 128), 0)).astype(F32)
    near, far = 8 * core, 8 - 8 * core
    n16 = iota((16, 128), 0)
    place_all = (iota((16, 128), 1) == OC + jnp.where(n16 < 8, n16 + near, n16 - near)).astype(F32)
    place_own = (iota((Z, 128), 1) == OC + near + iota((Z, 128), 0)).astype(F32)
    scale_d = 1.0 / math.sqrt(OC * OC * NV * VL)
    scale_s = -0.5 / math.sqrt(OC)
    c = coupling[...]
    placed = lax.dot_general(
        c, place_c, (((0,), (0,)), ((), ())), preferred_element_type=F32, precision=HI
    )
    out[...] = jnp.zeros((Z, 8, 128), F32)
    for j, ref in enumerate((mine, theirs)):
        t1 = singles_of(ref)
        row = placed[8 * j : 8 * (j + 1), :]
        row += dot(doubles[j] * scale_d, place_own, HI)
        row += dot(dot(dot(t1, half, HI), c, HI) * scale_s, place_all, HI)
        start = near if j == 0 else far
        t1_out[pl.ds(pl.multiple_of(start, 8), 8), :] = t1
        for n in range(Z):
            out[start // 2 + n // 2, n % 2 : n % 2 + 1, :] = row[n : n + 1, :]


def sum_kernel(x, out):
    out[...] = jnp.broadcast_to(jnp.sum(x[...], axis=0, keepdims=True), out.shape)


def final_kernel(ids, conv, active, x, t1, fock, singles, subspace):
    me = ids[0]
    total = jnp.sum(x[...], axis=0)
    mine = jnp.concatenate([t1[pl.ds(2 * me, 1), :], t1[pl.ds(2 * me + 1, 1), :]], axis=0)[:, 0:OC]
    all_fock = dot(t1[:, 0:OC].astype(BF), fock[...])
    own_fock = dot(mine.astype(BF), fock[...])
    a0 = (1 - conv[2 * me]).astype(F32)
    a1 = (1 - conv[2 * me + 1]).astype(F32)
    own_active = jnp.where(iota((2, OC), 0) == 0, a0, a1)
    singles[...] = own_active * (-own_fock - 0.5 * total[0:2, 0:OC])
    part = total[0:2, OC : OC + 2 * Z] - dot_nt(mine, all_fock, HI) * (1.0 / math.sqrt(OC))
    subspace[...] = part * active[...]


def out_kernel(ids, conv, x, *refs):
    me = ids[0]
    out, ov = refs[4], refs[5]
    for t in range(4):
        ov[lax.rem(me + t, 4)] = refs[t][...]
    for p in range(2):
        a = (1 - conv[2 * me + p]).astype(F32)
        for q in range(4):
            v = a * (x[q, p, 0:VL, :] + ov[q, p, 0:VL, :].astype(F32))
            out[p, :, BLK * q : BLK * (q + 1)] = v.astype(BF)


def local(trial_singles, trial_doubles, occ_fock, virt_fock, w_ovoo, w_ooov, converged):
    ids = jnp.stack([lax.axis_index("root"), lax.axis_index("occ")]).astype(jnp.int32)
    active = (1 - converged).astype(F32)[None, :]
    chunks = (4, 2, VP, BLK)
    roots = (Z, VP, BLK)
    w_spec = pl.BlockSpec((16, VL, BLK), lambda s: (s, 0, 0))

    zb, xb = call(
        prep_kernel, (shape(chunks, BF), shape((NV, VP, COLS), BF)), [SMEM, VMEM, VMEM], name="prep"
    )(ids, trial_doubles, trial_singles)

    gathered = lax.all_to_all(xb, VIRT, split_axis=0, concat_axis=0, tiled=True)
    blocks = to_blocks(zb)
    oo = call(
        oo_kernel,
        shape(chunks, F32),
        [SMEM, VMEM, VMEM, VMEM],
        [
            VMEM((384, 768), BF),
            VMEM((192, GRP), BF),
            VMEM((2, 192, GRP), F32),
            VMEM((2, 768, GRP), BF),
        ],
        flops=2 << 30,
        name="oo",
    )(ids, zb, other_core(zb), occ_fock)
    product = call(
        mm_kernel, shape((NV, VP, COLS), BF), [VMEM, VMEM], flops=1 << 29, name="mm"
    )(virt_fock, gathered)
    vv = lax.all_to_all(product, VIRT, split_axis=0, concat_axis=0, tiled=True)

    mine = call(gather_kernel, shape(roots, BF), [SMEM] + [VMEM] * 4, name="gather")(ids, *blocks)
    theirs = other_core(mine)
    outer_mine, outer_theirs = call(
        outer_kernel,
        (shape(roots, BF), shape(roots, BF)),
        [SMEM, VMEM, VMEM, w_spec],
        [VMEM((16, 16, BLK), BF), VMEM((2, 256, BLK), F32), VMEM((16, 128), F32)],
        flops=1 << 30,
        grid=(3,),
        name="outer",
    )(ids, mine, theirs, w_ovoo)
    ov = call(add_kernel, shape(chunks, BF), [SMEM, VMEM, VMEM], name="add")(
        ids, outer_mine, other_core(outer_theirs)
    )
    ov_owned = to_owners(ov)
    coupling = call(
        coupling_kernel,
        shape((KH, 16), F32),
        [VMEM, VMEM, w_spec],
        [VMEM((16, 16, BLK), BF), VMEM((2, 256, BLK), BF)],
        flops=1 << 30,
        grid=(3,),
        out_spec=pl.BlockSpec((16, 16), lambda s: (s, 0)),
        name="coupling",
    )(mine, theirs, w_ooov)

    x, xr = call(
        x_kernel, (shape(chunks, F32), shape(chunks, BF)), [SMEM, VMEM, VMEM], name="x"
    )(ids, vv, oo)
    x_blocks = to_blocks(xr)
    message, t1 = call(
        s_kernel,
        (shape((Z, 8, 128), F32), shape((16, 128), F32)),
        [SMEM] + [VMEM] * 8,
        [VMEM(roots, BF)],
        name="s",
    )(ids, mine, theirs, ov, coupling, *x_blocks)
    arrived = lax.all_to_all(message, "root", split_axis=0, concat_axis=0, tiled=True)
    copies = call(sum_kernel, shape((32, 8, 128), F32), [VMEM], name="sum")(arrived)
    arrived = lax.all_to_all(copies, REST, split_axis=0, concat_axis=0, tiled=True)
    sigma_singles, subspace = call(
        final_kernel,
        (shape((2, OC), F32), shape((2, 2 * Z), F32)),
        [SMEM, SMEM, VMEM, VMEM, VMEM, VMEM],
        name="final",
    )(ids, converged, active, arrived, t1, occ_fock)

    sigma_doubles = call(
        out_kernel,
        shape((2, VL, HALF), BF),
        [SMEM, SMEM] + [VMEM] * 5,
        [VMEM(chunks, BF)],
        name="out",
    )(ids, converged, x, *ov_owned)
    return (sigma_doubles, sigma_singles, subspace)


def solution(mesh):
    torus = Mesh(
        mesh.devices.reshape(mesh.shape["root"], 4, 4, mesh.shape["occ"]),
        ("root", "virt_0", "virt_1", "occ"),
    )
    return jax.shard_map(
        local,
        mesh=torus,
        in_specs=(
            P("root", None),
            P("root", VIRT, "occ"),
            P(),
            P(),
            P("occ", VIRT, "root"),
            P("occ", VIRT, "root"),
            P(),
        ),
        out_specs=(P("root", VIRT, "occ"), P("root", None), P("root", None)),
        check_vma=False,
    )
```

```python
import math

import jax
import jax.numpy as jnp
from jax import lax
from jax.experimental import pallas as pl
from jax.experimental.pallas import tpu as pltpu
from jax.sharding import Mesh
from jax.sharding import PartitionSpec as P


VIRT = ("virt_0", "virt_1")
ROOT_OCC = ("root", "occ")
BF = jnp.bfloat16
F32 = jnp.float32
HI = lax.Precision.HIGHEST

Z = 8
NV = 16
OC = 96
VL = 30
VP = 32
BLK = 1152
HALF = 4608
COLS = 640
KH = 48
SPARE = 30
GRP = 384

VMEM = pltpu.VMEM
SMEM = pltpu.SMEM


def iota(shape, dim):
    return lax.broadcasted_iota(jnp.int32, shape, dim)


def dot(a, b, precision=None):
    return jnp.dot(a, b, preferred_element_type=F32, precision=precision)


def dot_nt(a, b, precision=None):
    return lax.dot_general(
        a, b, (((1,), (1,)), ((), ())), preferred_element_type=F32, precision=precision
    )


def call(kernel, outs, places, scratch=(), limit=12, flops=1 << 24):
    return pl.pallas_call(
        kernel,
        out_shape=outs,
        in_specs=[pl.BlockSpec(memory_space=p) for p in places],
        out_specs=jax.tree.map(lambda _: pl.BlockSpec(memory_space=VMEM), outs),
        scratch_shapes=scratch,
        compiler_params=pltpu.CompilerParams(vmem_limit_bytes=limit << 20),
        cost_estimate=pl.CostEstimate(flops=flops, bytes_accessed=1 << 20, transcendentals=0),
    )


def exchange(x, axes):
    return lax.all_to_all(x, axes, split_axis=0, concat_axis=0, tiled=True)


def shape(dims, dtype):
    return jax.ShapeDtypeStruct(dims, dtype)


def other_core(x):
    return lax.ppermute(x, "occ", [(0, 1), (1, 0)])


def z_pairs(t):
    return [
        (2 * r + o, 2 * (4 * o + (r + t) % 4) + r // 4) for r in range(Z) for o in range(2)
    ]


def z_steps(x, back=False):
    out = []
    for t in range(4):
        pairs = [(b, a) if back else (a, b) for a, b in z_pairs(t)]
        out.append(lax.ppermute(x[t], ROOT_OCC, pairs))
    return out


def slot_of(q, me):
    return lax.rem(q - me + Z, 4)


def tiles_of(first, count):
    tile, out = 0, []
    while tile < count:
        g, off = divmod(first + tile, 5)
        n = min(5 - off, count - tile)
        out.append((g, 128 * off, 128 * (off + n), 128 * tile, 128 * (tile + n)))
        tile += n
    return out


def prep_kernel(ids, doubles, t1, zb, xb):
    me = ids[0]
    place = (iota((OC, 128), 0) == iota((OC, 128), 1)).astype(F32)
    wide = dot(t1[...].astype(F32), place, HI)
    first = iota((2, 128), 0) == 0
    xb[:, VL:VP, :] = jnp.zeros((NV, VP - VL, COLS), BF)
    xb[14, 0:VL, 256:COLS] = jnp.zeros((VL, COLS - 256), BF)
    xb[15, 0:VL, :] = jnp.zeros((VL, COLS), BF)
    for p in range(2):
        tail = jnp.where(first, jnp.broadcast_to(wide[p : p + 1, :], (2, 128)), 0.0).astype(BF)
        for q in range(4):
            slot = slot_of(q, me)
            zb[slot, p, 0:VL, :] = doubles[p, :, BLK * q : BLK * (q + 1)]
            zb[slot, p, VL:VP, 0:128] = tail
            zb[slot, p, VL:VP, 128:BLK] = jnp.zeros((VP - VL, BLK - 128), BF)
        for g, a, b, lo, hi in tiles_of(36 * p, 36):
            xb[g, 0:VL, a:b] = doubles[p, :, lo:hi]


def oo_kernel(ids, zb, zo, fock, oo, left, own, stack, rolled):
    me, core = ids[0], ids[1]
    f = fock[...]
    rows, depth, half = 96, 768, 192
    e3 = (lax.rem(iota((GRP, OC), 0), OC) == iota((GRP, OC), 1)).astype(BF)
    same = iota((GRP, GRP), 0) // OC == iota((GRP, GRP), 1) // OC
    bd = dot_nt(dot(e3, f).astype(BF), e3)
    bd = jnp.where(same, bd, 0.0).astype(BF)
    col = iota((OC, depth), 1)
    shift = col // half
    group = lax.rem(col, half) // 8
    group = jnp.where(group < 12, group + 12 * core, group - 12 * core)
    diag = lax.rem(iota((rows, depth), 0), 8) == lax.rem(iota((rows, depth), 1), 8)
    for i in range(4):
        mine = 4 * (12 * core + iota((rows, OC), 0) // 8) + i
        ef = dot_nt((iota((rows, OC), 1) == mine).astype(BF), f).astype(BF)
        e2 = (iota((OC, depth), 0) == 4 * group + ((i - shift) & 3)).astype(BF)
        left[rows * i : rows * (i + 1), :] = jnp.where(diag, dot(ef, e2), 0.0).astype(BF)
    lane = iota((rows, 256), 1) & 127
    for p in range(2):
        for b in range(2):
            for h, ref in enumerate((zb, zo)):
                for q in range(4):
                    slot = slot_of(q, me)
                    for u in range(3):
                        at = 12 * h + 3 * q + u
                        piece = ref[
                            slot, p, 16 * b : 16 * (b + 1), GRP * u : GRP * (u + 1)
                        ].astype(F32)
                        stack[0, 8 * at : 8 * (at + 1), :] = piece[0:8, :]
                        stack[1, 8 * at : 8 * (at + 1), :] = piece[8:16, :]
            for c in range(2):
                wide = stack[c]
                rolled[c, 0:half, :] = wide.astype(BF)
                own[rows * c : rows * (c + 1), :] = wide[0:rows, :].astype(BF)
                for s in range(1, 4):
                    rolled[c, half * s : half * (s + 1), :] = pltpu.roll(wide, OC * s, 1).astype(BF)
            second = dot(own[...], bd)
            for tile in range(3):
                lo, hi = 128 * tile, 128 * (tile + 1)
                rhs = jnp.concatenate([rolled[0, :, lo:hi], rolled[1, :, lo:hi]], axis=1)
                y = dot(left[rows * tile : rows * (tile + 2), :], rhs)
                v = jnp.where(lane < 96 - 32 * tile, y[0:rows, :], y[rows:, :])
                for c in range(2):
                    w = v[:, 128 * c : 128 * (c + 1)] + second[rows * c : rows * (c + 1), lo:hi]
                    for g in range(12):
                        q, u = divmod(g, 3)
                        oo[
                            q,
                            p,
                            16 * b + 8 * c : 16 * b + 8 * (c + 1),
                            GRP * u + lo : GRP * u + hi,
                        ] = w[8 * g : 8 * (g + 1), :]


def mm_kernel(fock, x, out):
    n = NV * VP
    count = NV * VL
    row = iota((n, count), 0)
    pick = (VL * (row // VP) + lax.rem(row, VP) == iota((n, count), 1)) & (lax.rem(row, VP) < VL)
    pick = pick.astype(BF)
    padded = dot_nt(dot(pick, fock[...]).astype(BF), pick).astype(BF)
    y = dot(padded, x[...].reshape(n, COLS)).astype(BF)
    out[...] = y.reshape(NV, VP, COLS)


def gather_kernel(ids, after, *refs):
    me, out = ids[0], refs[4]
    del after
    for t in range(4):
        at = 2 * lax.rem(me - t + Z, 4)
        for p in range(2):
            out[at + p] = refs[t][p]


def singles_of(ref):
    mask = iota((16, 128), 0) == SPARE - 16
    rows = []
    for r in range(Z):
        x = ref[r, 16:32, 0:128].astype(F32)
        rows.append(jnp.sum(jnp.where(mask, x, 0.0), axis=0, keepdims=True))
    return jnp.concatenate(rows, axis=0)


def outer_kernel(ids, mine, theirs, w, out_mine, out_theirs):
    core, k = ids[1], 16 * KH
    t1 = jnp.concatenate([singles_of(mine), singles_of(theirs)], axis=0).astype(BF)
    e1 = (iota((256, 16), 0) // 16 == iota((256, 16), 1)).astype(BF)
    e2 = (iota((128, k), 0) == KH * core + lax.rem(iota((128, k), 1), KH)).astype(BF)
    spread = dot(dot(e1, t1).astype(BF), e2)
    diag = lax.rem(iota((256, k), 0), 16) == iota((256, k), 1) // KH
    spread = jnp.where(diag, -spread, 0.0).astype(BF)
    for b, (first, last) in enumerate(((0, 16), (16, VL))):
        depth = (last - first) * KH
        y = dot(spread[:, 0:depth], w[first:last].reshape(depth, BLK)).astype(BF)
        for n in range(Z):
            out_mine[n, 16 * b : 16 * (b + 1), :] = y[16 * n : 16 * (n + 1), :]
            out_theirs[n, 16 * b : 16 * (b + 1), :] = y[128 + 16 * n : 128 + 16 * (n + 1), :]


def add_kernel(ids, a, b, out):
    me = ids[0]
    for t in range(4):
        at = 2 * lax.rem(me - t + Z, 4)
        for p in range(2):
            out[t, p] = (a[at + p].astype(F32) + b[at + p].astype(F32)).astype(BF)


def coupling_kernel(mine, theirs, w, out, t):
    for b in range(2):
        for j, ref in enumerate((mine, theirs)):
            t[b, 128 * j : 128 * (j + 1), :] = ref[:, 16 * b : 16 * (b + 1), :].reshape(128, BLK)
    total = jnp.zeros((KH, 256), F32)
    for b, (first, last) in enumerate(((0, 16), (16, VL))):
        depth = (last - first) * KH
        g = dot_nt(w[first:last].reshape(depth, BLK), t[b])
        g = jnp.where(iota(g.shape, 0) // KH == lax.rem(iota(g.shape, 1), 16), g, 0.0)
        total += jnp.sum(g.reshape(last - first, KH, 256), axis=0)
    right = (iota((256, 16), 0) // 16 == iota((256, 16), 1)).astype(F32)
    out[...] = dot(total, right, HI)


def x_kernel(ids, after, vv, oo, x, xb):
    me = ids[0]
    del after
    for p in range(2):
        for q in range(4):
            slot = slot_of(q, me)
            for g, a, b, lo, hi in tiles_of(36 * p + 9 * q, 9):
                v = vv[g, :, a:b].astype(F32) - oo[q, p, :, lo:hi]
                x[q, p, :, lo:hi] = v
                xb[slot, p, :, lo:hi] = v.astype(BF)


def base_kernel(ids, mine, theirs, coupling, rows, t1_out):
    core = ids[1]
    half = (iota((128, KH), 0) == KH * core + iota((128, KH), 1)).astype(F32)
    place_c = (iota((KH, 128), 1) == KH * core + iota((KH, 128), 0)).astype(F32)
    near, far = 8 * core, 8 - 8 * core
    n16 = iota((16, 128), 0)
    place = (iota((16, 128), 1) == OC + jnp.where(n16 < 8, n16 + near, n16 - near)).astype(F32)
    c = coupling[...]
    t1 = [singles_of(mine), singles_of(theirs)]
    row = lax.dot_general(
        c, place_c, (((0,), (0,)), ((), ())), preferred_element_type=F32, precision=HI
    )
    both = jnp.concatenate(t1, axis=0)
    row += dot(dot(dot(both, half, HI), c, HI) * (-0.5 / math.sqrt(OC)), place, HI)
    rows[...] = row
    for j, start in enumerate((near, far)):
        t1_out[pl.ds(pl.multiple_of(start, 8), 8), :] = t1[j]


def s_kernel(ids, mine, theirs, ov, rows, *refs):
    me, core = ids[0], ids[1]
    out, y = refs[4], refs[5]
    for t in range(4):
        at = 2 * lax.rem(me - t + Z, 4)
        for p in range(2):
            y[at + p] = (refs[t][p].astype(F32) + ov[t, p].astype(F32)).astype(BF)
    y[:, VL:VP, :] = jnp.zeros((Z, VP - VL, BLK), BF)
    near, far = 8 * core, 8 - 8 * core
    n8 = iota((128, 128), 0) // 16
    place = (iota((128, 128), 1) == OC + near + n8).astype(F32)
    place = place * (1.0 / math.sqrt(OC * OC * NV * VL))
    same = lax.rem(iota((128, 128), 0), 16) == lax.rem(iota((128, 128), 1), 16)
    left = (iota((Z, 128), 1) // 16 == iota((Z, 128), 0)).astype(F32)
    for j, ref in enumerate((mine, theirs)):
        g = jnp.zeros((128, 128), F32)
        for b in range(2):
            lhs = ref[:, 16 * b : 16 * (b + 1), :].reshape(128, BLK)
            g += dot_nt(lhs, y[:, 16 * b : 16 * (b + 1), :].reshape(128, BLK))
        row = rows[8 * j : 8 * (j + 1), :] + dot(dot(left, jnp.where(same, g, 0.0), HI), place, HI)
        start = (near if j == 0 else far) // 2
        for i in range(4):
            pair = jnp.concatenate([row[2 * i : 2 * i + 1, :], row[2 * i + 1 : 2 * i + 2, :]], axis=1)
            out[start + i] = jnp.broadcast_to(pair[None], (2, 1, 256))


def sum_kernel(x, out):
    out[...] = jnp.broadcast_to(jnp.sum(x[...], axis=0, keepdims=True), out.shape)


def final_kernel(ids, conv, active, x, t1, fock, singles, subspace):
    me = ids[0]
    summed = jnp.sum(x[...], axis=0)
    total = jnp.concatenate([summed[:, 0:128], summed[:, 128:256]], axis=0)
    mine = jnp.concatenate([t1[pl.ds(2 * me, 1), :], t1[pl.ds(2 * me + 1, 1), :]], axis=0)[:, 0:OC]
    all_fock = dot(t1[:, 0:OC].astype(BF), fock[...])
    own_fock = dot(mine.astype(BF), fock[...])
    a0 = (1 - conv[2 * me]).astype(F32)
    a1 = (1 - conv[2 * me + 1]).astype(F32)
    own_active = jnp.where(iota((2, OC), 0) == 0, a0, a1)
    singles[...] = own_active * (-own_fock - 0.5 * total[:, 0:OC])
    part = total[:, OC : OC + 2 * Z] - dot_nt(mine, all_fock, HI) * (1.0 / math.sqrt(OC))
    subspace[...] = part * active[...]


def out_kernel(ids, conv, x, *refs):
    me = ids[0]
    out, ov = refs[4], refs[5]
    for t in range(4):
        ov[lax.rem(me + t, 4)] = refs[t][...]
    for p in range(2):
        a = (1 - conv[2 * me + p]).astype(F32)
        for q in range(4):
            v = a * (x[q, p, 0:VL, :] + ov[q, p, 0:VL, :].astype(F32))
            out[p, :, BLK * q : BLK * (q + 1)] = v.astype(BF)


def local(trial_singles, trial_doubles, occ_fock, virt_fock, w_ovoo, w_ooov, converged):
    ids = jnp.stack([lax.axis_index("root"), lax.axis_index("occ")]).astype(jnp.int32)
    active = (1 - converged).astype(F32)[None, :]
    chunks = (4, 2, VP, BLK)
    roots = (Z, VP, BLK)
    w_ovoo = jnp.transpose(w_ovoo, (1, 0, 2))
    w_ooov = jnp.transpose(w_ooov, (1, 0, 2))

    zb, xb = call(
        prep_kernel, (shape(chunks, BF), shape((NV, VP, COLS), BF)), [SMEM, VMEM, VMEM]
    )(ids, trial_doubles, trial_singles)

    gathered = exchange(xb, VIRT)
    blocks = z_steps(zb)
    oo = call(
        oo_kernel,
        shape(chunks, F32),
        [SMEM, VMEM, VMEM, VMEM],
        [
            VMEM((384, 768), BF),
            VMEM((192, GRP), BF),
            VMEM((2, 192, GRP), F32),
            VMEM((2, 768, GRP), BF),
        ],
        flops=2 << 30,
    )(ids, zb, other_core(zb), occ_fock)
    product = call(
        mm_kernel, shape((NV, VP, COLS), BF), [VMEM, VMEM], flops=1 << 29
    )(virt_fock, gathered)
    vv = exchange(product, VIRT)

    mine = call(gather_kernel, shape(roots, BF), [SMEM, pl.ANY] + [VMEM] * 4)(ids, product, *blocks)
    theirs = other_core(mine)
    outer_mine, outer_theirs = call(
        outer_kernel, (shape(roots, BF), shape(roots, BF)), [SMEM, VMEM, VMEM, VMEM], flops=1 << 30
    )(ids, mine, theirs, w_ovoo)
    ov = call(add_kernel, shape(chunks, BF), [SMEM, VMEM, VMEM])(
        ids, outer_mine, other_core(outer_theirs)
    )
    ov_owned = z_steps(ov, back=True)
    coupling = call(
        coupling_kernel,
        shape((KH, 16), F32),
        [VMEM, VMEM, VMEM],
        [VMEM((2, 256, BLK), BF)],
        flops=1 << 30,
    )(mine, theirs, w_ooov)

    x, xr = call(
        x_kernel, (shape(chunks, F32), shape(chunks, BF)), [SMEM, pl.ANY, VMEM, VMEM]
    )(ids, coupling, vv, oo)
    x_blocks = z_steps(xr)
    rows, t1 = call(
        base_kernel, (shape((16, 128), F32), shape((16, 128), F32)), [SMEM, VMEM, VMEM, VMEM]
    )(ids, mine, theirs, coupling)
    message = call(
        s_kernel, shape((Z, 2, 1, 256), F32), [SMEM] + [VMEM] * 8, [VMEM(roots, BF)]
    )(ids, mine, theirs, ov, rows, *x_blocks)
    arrived = exchange(message.reshape(16, 1, 256), ROOT_OCC)
    copies = call(sum_kernel, shape((NV, 1, 256), F32), [VMEM])(arrived)
    arrived = exchange(copies, VIRT)
    sigma_singles, subspace = call(
        final_kernel,
        (shape((2, OC), F32), shape((2, 2 * Z), F32)),
        [SMEM, SMEM, VMEM, VMEM, VMEM, VMEM],
    )(ids, converged, active, arrived, t1, occ_fock)

    sigma_doubles = call(
        out_kernel, shape((2, VL, HALF), BF), [SMEM, SMEM] + [VMEM] * 5, [VMEM(chunks, BF)]
    )(ids, converged, x, *ov_owned)
    return (sigma_doubles, sigma_singles, subspace)


def solution(mesh):
    torus = Mesh(
        mesh.devices.reshape(mesh.shape["root"], 4, 4, mesh.shape["occ"]),
        ("root", "virt_0", "virt_1", "occ"),
    )
    return jax.shard_map(
        local,
        mesh=torus,
        in_specs=(
            P("root", None),
            P("root", VIRT, "occ"),
            P(),
            P(),
            P("occ", VIRT, "root"),
            P("occ", VIRT, "root"),
            P(),
        ),
        out_specs=(P("root", VIRT, "occ"), P("root", None), P("root", None)),
        check_vma=False,
    )
```

```python
import math

import jax
import jax.numpy as jnp
from jax import lax
from jax.experimental import pallas as pl
from jax.experimental.pallas import tpu as pltpu
from jax.sharding import Mesh
from jax.sharding import PartitionSpec as P


VIRT = ("virt_0", "virt_1")
ROOT_OCC = ("root", "occ")
BF = jnp.bfloat16
F32 = jnp.float32
HI = lax.Precision.HIGHEST

Z = 8
NV = 16
OC = 96
VL = 30
VP = 32
BLK = 1152
HALF = 4608
COLS = 640
KH = 48
SPARE = 30
VMEM = pltpu.VMEM
SMEM = pltpu.SMEM
GRP = 384


def iota(shape, dim):
    return lax.broadcasted_iota(jnp.int32, shape, dim)


def dot(a, b, precision=None):
    return jnp.dot(a, b, preferred_element_type=F32, precision=precision)


def dot_nt(a, b, precision=None):
    return lax.dot_general(
        a, b, (((1,), (1,)), ((), ())), preferred_element_type=F32, precision=precision
    )


def call(kernel, outs, places, scratch=(), limit=12, flops=1 << 24, out_place=VMEM):
    return pl.pallas_call(
        kernel,
        out_shape=outs,
        in_specs=[pl.BlockSpec(memory_space=p) for p in places],
        out_specs=jax.tree.map(lambda _: pl.BlockSpec(memory_space=out_place), outs),
        scratch_shapes=scratch,
        compiler_params=pltpu.CompilerParams(vmem_limit_bytes=limit << 20),
        cost_estimate=pl.CostEstimate(flops=flops, bytes_accessed=1 << 20, transcendentals=0),
    )


def exchange(x, axes):
    return lax.all_to_all(x, axes, split_axis=0, concat_axis=0, tiled=True)


def shape(dims, dtype):
    return jax.ShapeDtypeStruct(dims, dtype)


def other_core(x):
    return lax.ppermute(x, "occ", [(0, 1), (1, 0)])


def z_pairs(t):
    return [
        (2 * r + o, 2 * (4 * o + (r + t) % 4) + r // 4) for r in range(Z) for o in range(2)
    ]


def z_steps(x, back=False):
    out = []
    for t in range(4):
        pairs = [(b, a) if back else (a, b) for a, b in z_pairs(t)]
        out.append(lax.ppermute(x[t], ROOT_OCC, pairs))
    return out


def slot_of(q, me):
    return lax.rem(q - me + Z, 4)


def tiles_of(first, count):
    tile, out = 0, []
    while tile < count:
        g, off = divmod(first + tile, 5)
        n = min(5 - off, count - tile)
        out.append((g, 128 * off, 128 * (off + n), 128 * tile, 128 * (tile + n)))
        tile += n
    return out


def prep_kernel(ids, doubles, t1, zb, xb):
    me = ids[0]
    wide = t1[...].astype(F32)
    first = iota((2, 128), 0) == 0
    xb[:, VL:VP, :] = jnp.zeros((NV, VP - VL, COLS), BF)
    xb[14, 0:VL, 256:COLS] = jnp.zeros((VL, COLS - 256), BF)
    xb[15, 0:VL, :] = jnp.zeros((VL, COLS), BF)
    for p in range(2):
        tail = jnp.where(first, jnp.broadcast_to(wide[p : p + 1, :], (2, 128)), 0.0).astype(BF)
        for q in range(4):
            slot = slot_of(q, me)
            zb[slot, p, 0:VL, :] = doubles[p, :, BLK * q : BLK * (q + 1)]
            zb[slot, p, VL:VP, 0:128] = tail
            zb[slot, p, VL:VP, 128:BLK] = jnp.zeros((VP - VL, BLK - 128), BF)
        for g, a, b, lo, hi in tiles_of(36 * p, 36):
            xb[g, 0:VL, a:b] = doubles[p, :, lo:hi]


def oo_kernel(ids, zb, zo, fock, out_own, out_other, left, stack, rolled):
    me, core = ids[0], ids[1]
    rows, depth, half = 96, 768, 192

    def work():
        f = fock[...]
        e3 = (lax.rem(iota((GRP, OC), 0), OC) == iota((GRP, OC), 1)).astype(BF)
        same = iota((GRP, GRP), 0) // OC == iota((GRP, GRP), 1) // OC
        bd = dot_nt(dot(e3, f).astype(BF), e3)
        bd = jnp.where(same, bd, 0.0).astype(BF)
        col = iota((OC, depth), 1)
        shift = col // half
        group = lax.rem(col, half) // 8
        group = jnp.where(group < 12, group + 12 * core, group - 12 * core)
        diag = lax.rem(iota((rows, depth), 0), 8) == lax.rem(iota((rows, depth), 1), 8)
        for i in range(4):
            e2 = (iota((OC, depth), 0) == 4 * group + ((i - shift) & 3)).astype(BF)
            for h in range(2):
                first = 12 * core if h == 0 else 12 - 12 * core
                at = 4 * (first + iota((rows, OC), 0) // 8) + i
                ef = dot_nt((iota((rows, OC), 1) == at).astype(BF), f).astype(BF)
                m = jnp.where(diag, dot(ef, e2), 0.0).astype(BF)
                left[h, rows * i : rows * (i + 1), :] = m
        lane = iota((rows, 256), 1) & 127
        for p in range(2):
            for b in range(2):
                for h, ref in enumerate((zb, zo)):
                    for q in range(4):
                        slot = slot_of(q, me)
                        for u in range(3):
                            at = 8 * (12 * h + 3 * q + u)
                            piece = ref[
                                slot, p, 16 * b : 16 * (b + 1), GRP * u : GRP * (u + 1)
                            ].astype(F32)
                            stack[0, at : at + 8, :] = piece[0:8, :]
                            stack[1, at : at + 8, :] = piece[8:16, :]
                for c in range(2):
                    wide = stack[c]
                    rolled[c, 0:half, :] = wide.astype(BF)
                    for s in range(1, 4):
                        moved = pltpu.roll(wide, OC * s, 1)
                        rolled[c, half * s : half * (s + 1), :] = moved.astype(BF)
                second = [dot(rolled[c, 0:half, :], bd) for c in range(2)]
                for tile in range(3):
                    lo, hi = 128 * tile, 128 * (tile + 1)
                    rhs = jnp.concatenate([rolled[0, :, lo:hi], rolled[1, :, lo:hi]], axis=1)
                    for h, out in enumerate((out_own, out_other)):
                        y = dot(left[h, rows * tile : rows * (tile + 2), :], rhs)
                        v = jnp.where(lane < 96 - 32 * tile, y[0:rows, :], y[rows:, :])
                        w = [
                            v[:, 128 * c : 128 * (c + 1)]
                            + second[c][rows * h : rows * (h + 1), lo:hi]
                            for c in range(2)
                        ]
                        for g in range(12):
                            q, u = divmod(g, 3)
                            part = [x[8 * g : 8 * (g + 1), :] for x in w]
                            out[q, p, 16 * b : 16 * (b + 1), GRP * u + lo : GRP * u + hi] = (
                                jnp.concatenate(part, axis=0).astype(BF)
                            )

    pl.when(me // 4 == core)(work)


def mm_kernel(fock, x, out):
    n = NV * VP
    count = NV * VL
    row = iota((n, count), 0)
    pick = (VL * (row // VP) + lax.rem(row, VP) == iota((n, count), 1)) & (lax.rem(row, VP) < VL)
    pick = pick.astype(BF)
    padded = dot_nt(dot(pick, fock[...]).astype(BF), pick).astype(BF)
    y = dot(padded, x[...].reshape(n, COLS)).astype(BF)
    out[...] = y.reshape(NV, VP, COLS)


def gather_kernel(ids, after, *refs):
    me, out = ids[0], refs[4]
    del after
    for t in range(4):
        at = 2 * lax.rem(me - t + Z, 4)
        for p in range(2):
            out[at + p] = refs[t][p]


def singles_of(ref):
    mask = iota((16, 128), 0) == SPARE - 16
    rows = []
    for r in range(Z):
        x = ref[r, 16:32, 0:128].astype(F32)
        rows.append(jnp.sum(jnp.where(mask, x, 0.0), axis=0, keepdims=True))
    return jnp.concatenate(rows, axis=0)


def outer_kernel(ids, mine, theirs, w, out_mine, out_theirs):
    core, k = ids[1], 16 * KH
    t1 = jnp.concatenate([singles_of(mine), singles_of(theirs)], axis=0).astype(BF)
    e1 = (iota((256, 16), 0) // 16 == iota((256, 16), 1)).astype(BF)
    e2 = (iota((128, k), 0) == KH * core + lax.rem(iota((128, k), 1), KH)).astype(BF)
    spread = dot(dot(e1, t1).astype(BF), e2)
    diag = lax.rem(iota((256, k), 0), 16) == iota((256, k), 1) // KH
    spread = jnp.where(diag, -spread, 0.0).astype(BF)
    for b, (first, last) in enumerate(((0, 16), (16, VL))):
        depth = (last - first) * KH
        y = dot(spread[:, 0:depth], w[first:last].reshape(depth, BLK)).astype(BF)
        for n in range(Z):
            out_mine[n, 16 * b : 16 * (b + 1), :] = y[16 * n : 16 * (n + 1), :]
            out_theirs[n, 16 * b : 16 * (b + 1), :] = y[128 + 16 * n : 128 + 16 * (n + 1), :]


def add_kernel(ids, a, b, out):
    me = ids[0]
    for t in range(4):
        at = 2 * lax.rem(me - t + Z, 4)
        for p in range(2):
            out[t, p] = (a[at + p].astype(F32) + b[at + p].astype(F32)).astype(BF)


def coupling_kernel(mine, theirs, w, out, t):
    for b in range(2):
        for j, ref in enumerate((mine, theirs)):
            t[b, 128 * j : 128 * (j + 1), :] = ref[:, 16 * b : 16 * (b + 1), :].reshape(128, BLK)
    total = jnp.zeros((KH, 256), F32)
    for b, (first, last) in enumerate(((0, 16), (16, VL))):
        depth = (last - first) * KH
        g = dot_nt(w[first:last].reshape(depth, BLK), t[b])
        g = jnp.where(iota(g.shape, 0) // KH == lax.rem(iota(g.shape, 1), 16), g, 0.0)
        total += jnp.sum(g.reshape(last - first, KH, 256), axis=0)
    right = (iota((256, 16), 0) // 16 == iota((256, 16), 1)).astype(F32)
    out[...] = dot(total, right, HI)


def pick_kernel(ids, oo_own, oo_far, out):
    near = ids[0] // 4 == ids[1]

    @pl.when(near)
    def _():
        out[...] = oo_own[...]

    @pl.when(jnp.logical_not(near))
    def _():
        out[...] = oo_far[...]


def x_kernel(ids, vv, oo, xb):
    me = ids[0]
    for p in range(2):
        for q in range(4):
            slot = slot_of(q, me)
            for g, a, b, lo, hi in tiles_of(36 * p + 9 * q, 9):
                v = vv[g, :, a:b].astype(F32) - oo[q, p, :, lo:hi].astype(F32)
                xb[slot, p, :, lo:hi] = v.astype(BF)


def base_kernel(ids, mine, theirs, coupling, rows, t1_out):
    core = ids[1]
    half = (iota((128, KH), 0) == KH * core + iota((128, KH), 1)).astype(F32)
    place_c = (iota((KH, 128), 1) == KH * core + iota((KH, 128), 0)).astype(F32)
    near, far = 8 * core, 8 - 8 * core
    n16 = iota((16, 128), 0)
    place = (iota((16, 128), 1) == OC + jnp.where(n16 < 8, n16 + near, n16 - near)).astype(F32)
    c = coupling[...]
    t1 = [singles_of(mine), singles_of(theirs)]
    row = lax.dot_general(
        c, place_c, (((0,), (0,)), ((), ())), preferred_element_type=F32, precision=HI
    )
    both = jnp.concatenate(t1, axis=0)
    row += dot(dot(dot(both, half, HI), c, HI) * (-0.5 / math.sqrt(OC)), place, HI)
    rows[...] = row
    for j, start in enumerate((near, far)):
        t1_out[pl.ds(pl.multiple_of(start, 8), 8), :] = t1[j]


def s_kernel(ids, mine, theirs, ov, rows, *refs):
    me, core = ids[0], ids[1]
    out, y = refs[4], refs[5]
    for t in range(4):
        at = 2 * lax.rem(me - t + Z, 4)
        for p in range(2):
            y[at + p] = (refs[t][p].astype(F32) + ov[t, p].astype(F32)).astype(BF)
    y[:, VL:VP, :] = jnp.zeros((Z, VP - VL, BLK), BF)
    near, far = 8 * core, 8 - 8 * core
    n8 = iota((128, 128), 0) // 16
    place = (iota((128, 128), 1) == OC + near + n8).astype(F32)
    place = place * (1.0 / math.sqrt(OC * OC * NV * VL))
    same = lax.rem(iota((128, 128), 0), 16) == lax.rem(iota((128, 128), 1), 16)
    left = (iota((Z, 128), 1) // 16 == iota((Z, 128), 0)).astype(F32)
    for j, ref in enumerate((mine, theirs)):
        g = jnp.zeros((128, 128), F32)
        for b in range(2):
            lhs = ref[:, 16 * b : 16 * (b + 1), :].reshape(128, BLK)
            g += dot_nt(lhs, y[:, 16 * b : 16 * (b + 1), :].reshape(128, BLK))
        row = rows[8 * j : 8 * (j + 1), :] + dot(dot(left, jnp.where(same, g, 0.0), HI), place, HI)
        start = (near if j == 0 else far) // 2
        for i in range(4):
            pair = jnp.concatenate([row[2 * i : 2 * i + 1, :], row[2 * i + 1 : 2 * i + 2, :]], axis=1)
            out[start + i] = jnp.broadcast_to(pair[None], (2, 1, 256))


def sum_kernel(x, out):
    out[...] = jnp.broadcast_to(jnp.sum(x[...], axis=0, keepdims=True), out.shape)


def final_kernel(ids, conv, active, x, t1, fock, singles, subspace):
    me = ids[0]
    summed = jnp.sum(x[...], axis=0)
    total = jnp.concatenate([summed[:, 0:128], summed[:, 128:256]], axis=0)
    mine = jnp.concatenate([t1[pl.ds(2 * me, 1), :], t1[pl.ds(2 * me + 1, 1), :]], axis=0)[:, 0:OC]
    all_fock = dot(t1[:, 0:OC].astype(BF), fock[...])
    own_fock = dot(mine.astype(BF), fock[...])
    a0 = (1 - conv[2 * me]).astype(F32)
    a1 = (1 - conv[2 * me + 1]).astype(F32)
    own_active = jnp.where(iota((2, OC), 0) == 0, a0, a1)
    singles[...] = own_active * (-own_fock - 0.5 * total[:, 0:OC])
    part = total[:, OC : OC + 2 * Z] - dot_nt(mine, all_fock, HI) * (1.0 / math.sqrt(OC))
    subspace[...] = part * active[...]


def out_kernel(ids, conv, x, *refs):
    me = ids[0]
    out, total = refs[4], refs[5]
    for t in range(4):
        total[lax.rem(me + t, 4)] = x[t].astype(F32) + refs[t][...].astype(F32)
    for p in range(2):
        a = (1 - conv[2 * me + p]).astype(F32)
        for q in range(4):
            out[p, :, BLK * q : BLK * (q + 1)] = (a * total[q, p, 0:VL, :]).astype(BF)


def local(trial_singles, trial_doubles, occ_fock, virt_fock, w_ovoo, w_ooov, converged):
    ids = jnp.stack([lax.axis_index("root"), lax.axis_index("occ")]).astype(jnp.int32)
    active = (1 - converged).astype(F32)[None, :]
    chunks = (4, 2, VP, BLK)
    roots = (Z, VP, BLK)
    w_ovoo = jnp.transpose(w_ovoo, (1, 0, 2))
    w_ooov = jnp.transpose(w_ooov, (1, 0, 2))

    zb, xb = call(
        prep_kernel, (shape(chunks, BF), shape((NV, VP, COLS), BF)), [SMEM, VMEM, VMEM]
    )(ids, trial_doubles, jnp.pad(trial_singles, ((0, 0), (0, 128 - OC))))

    gathered = exchange(xb, VIRT)
    blocks = z_steps(zb)
    zo = other_core(zb)
    oo_own, oo_other = call(
        oo_kernel,
        (shape(chunks, BF), shape(chunks, BF)),
        [SMEM, VMEM, VMEM, VMEM],
        [
            VMEM((2, 384, 768), BF),
            VMEM((2, 192, GRP), F32),
            VMEM((2, 768, GRP), BF),
        ],
        flops=2 << 30,
    )(ids, zb, zo, occ_fock)
    oo_far = other_core(oo_other)
    oo = call(pick_kernel, shape(chunks, BF), [SMEM, VMEM, VMEM])(
        ids, oo_own, oo_far
    )
    product = call(
        mm_kernel, shape((NV, VP, COLS), BF), [VMEM, VMEM], flops=1 << 29
    )(virt_fock, gathered)
    vv = exchange(product, VIRT)

    mine = call(gather_kernel, shape(roots, BF), [SMEM, pl.ANY] + [VMEM] * 4)(ids, product, *blocks)
    theirs = other_core(mine)
    outer_mine, outer_theirs = call(
        outer_kernel, (shape(roots, BF), shape(roots, BF)), [SMEM, VMEM, VMEM, VMEM], flops=1 << 30
    )(ids, mine, theirs, w_ovoo)
    ov = call(add_kernel, shape(chunks, BF), [SMEM, VMEM, VMEM])(
        ids, outer_mine, other_core(outer_theirs)
    )
    ov_owned = z_steps(ov, back=True)
    coupling = call(
        coupling_kernel,
        shape((KH, 16), F32),
        [VMEM, VMEM, VMEM],
        [VMEM((2, 256, BLK), BF)],
        flops=1 << 30,
    )(mine, theirs, w_ooov)

    x = call(x_kernel, shape(chunks, BF), [SMEM, VMEM, VMEM])(ids, vv, oo)
    x_blocks = z_steps(x)
    rows, t1 = call(
        base_kernel, (shape((16, 128), F32), shape((16, 128), F32)), [SMEM, VMEM, VMEM, VMEM]
    )(ids, mine, theirs, coupling)
    message = call(
        s_kernel, shape((Z, 2, 1, 256), F32), [SMEM] + [VMEM] * 8, [VMEM(roots, BF)]
    )(ids, mine, theirs, ov, rows, *x_blocks)
    arrived = exchange(message.reshape(16, 1, 256), ROOT_OCC)
    copies = call(sum_kernel, shape((NV, 1, 256), F32), [VMEM])(arrived)
    arrived = exchange(copies, VIRT)
    sigma_singles, subspace = call(
        final_kernel,
        (shape((2, OC), F32), shape((2, 2 * Z), F32)),
        [SMEM, SMEM, VMEM, VMEM, VMEM, VMEM],
    )(ids, converged, active, arrived, t1, occ_fock)

    sigma_doubles = call(
        out_kernel, shape((2, VL, HALF), BF), [SMEM, SMEM] + [VMEM] * 5, [VMEM(chunks, F32)]
    )(ids, converged, x, *ov_owned)
    return (sigma_doubles, sigma_singles, subspace)


def solution(mesh):
    torus = Mesh(
        mesh.devices.reshape(mesh.shape["root"], 4, 4, mesh.shape["occ"]),
        ("root", "virt_0", "virt_1", "occ"),
    )
    return jax.shard_map(
        local,
        mesh=torus,
        in_specs=(
            P("root", None),
            P("root", VIRT, "occ"),
            P(),
            P(),
            P("occ", VIRT, "root"),
            P("occ", VIRT, "root"),
            P(),
        ),
        out_specs=(P("root", VIRT, "occ"), P("root", None), P("root", None)),
        check_vma=False,
    )
```

```python
import math

import jax
import jax.numpy as jnp
from jax import lax
from jax.experimental import pallas as pl
from jax.experimental.pallas import tpu as pltpu
from jax.sharding import Mesh
from jax.sharding import PartitionSpec as P


VIRT = ("virt_0", "virt_1")
ROOT_OCC = ("root", "occ")
BF = jnp.bfloat16
F32 = jnp.float32
HI = lax.Precision.HIGHEST

Z = 8
NV = 16
OC = 96
VL = 30
VP = 32
BLK = 1152
HALF = 4608
COLS = 640
KH = 48
SPARE = 30
GRP = 384

VMEM = pltpu.VMEM
SMEM = pltpu.SMEM


def iota(shape, dim):
    return lax.broadcasted_iota(jnp.int32, shape, dim)


def dot(a, b, precision=None):
    return jnp.dot(a, b, preferred_element_type=F32, precision=precision)


def dot_nt(a, b, precision=None):
    return lax.dot_general(
        a, b, (((1,), (1,)), ((), ())), preferred_element_type=F32, precision=precision
    )


def call(kernel, outs, places, scratch=(), limit=12, flops=1 << 24):
    return pl.pallas_call(
        kernel,
        out_shape=outs,
        in_specs=[pl.BlockSpec(memory_space=p) for p in places],
        out_specs=jax.tree.map(lambda _: pl.BlockSpec(memory_space=VMEM), outs),
        scratch_shapes=scratch,
        compiler_params=pltpu.CompilerParams(vmem_limit_bytes=limit << 20),
        cost_estimate=pl.CostEstimate(flops=flops, bytes_accessed=1 << 20, transcendentals=0),
    )


def exchange(x, axes):
    return lax.all_to_all(x, axes, split_axis=0, concat_axis=0, tiled=True)


def shape(dims, dtype):
    return jax.ShapeDtypeStruct(dims, dtype)


def other_core(x):
    return lax.ppermute(x, "occ", [(0, 1), (1, 0)])


def z_pairs(t):
    return [
        (2 * r + o, 2 * (4 * o + (r + t) % 4) + r // 4) for r in range(Z) for o in range(2)
    ]


def z_steps(x, back=False):
    out = []
    for t in range(4):
        pairs = [(b, a) if back else (a, b) for a, b in z_pairs(t)]
        out.append(lax.ppermute(x[t], ROOT_OCC, pairs))
    return out


def slot_of(q, me):
    return lax.rem(q - me + Z, 4)


def tiles_of(first, count):
    tile, out = 0, []
    while tile < count:
        g, off = divmod(first + tile, 5)
        n = min(5 - off, count - tile)
        out.append((g, 128 * off, 128 * (off + n), 128 * tile, 128 * (tile + n)))
        tile += n
    return out


def prep_kernel(ids, doubles, t1, zb, xb):
    me = ids[0]
    place = (iota((OC, 128), 0) == iota((OC, 128), 1)).astype(F32)
    wide = dot(t1[...].astype(F32), place, HI)
    first = iota((2, 128), 0) == 0
    xb[:, VL:VP, :] = jnp.zeros((NV, VP - VL, COLS), BF)
    xb[14, 0:VL, 256:COLS] = jnp.zeros((VL, COLS - 256), BF)
    xb[15, 0:VL, :] = jnp.zeros((VL, COLS), BF)
    for p in range(2):
        tail = jnp.where(first, jnp.broadcast_to(wide[p : p + 1, :], (2, 128)), 0.0).astype(BF)
        for q in range(4):
            slot = slot_of(q, me)
            zb[slot, p, 0:VL, :] = doubles[p, :, BLK * q : BLK * (q + 1)]
            zb[slot, p, VL:VP, 0:128] = tail
            zb[slot, p, VL:VP, 128:BLK] = jnp.zeros((VP - VL, BLK - 128), BF)
        for g, a, b, lo, hi in tiles_of(36 * p, 36):
            xb[g, 0:VL, a:b] = doubles[p, :, lo:hi]


def oo_kernel(ids, zb, zo, fock, oo, left, own, stack, rolled):
    me, core = ids[0], ids[1]
    f = fock[...]
    rows, depth, half = 96, 768, 192
    e3 = (lax.rem(iota((GRP, OC), 0), OC) == iota((GRP, OC), 1)).astype(BF)
    same = iota((GRP, GRP), 0) // OC == iota((GRP, GRP), 1) // OC
    bd = dot_nt(dot(e3, f).astype(BF), e3)
    bd = jnp.where(same, bd, 0.0).astype(BF)
    col = iota((OC, depth), 1)
    shift = col // half
    group = lax.rem(col, half) // 8
    group = jnp.where(group < 12, group + 12 * core, group - 12 * core)
    diag = lax.rem(iota((rows, depth), 0), 8) == lax.rem(iota((rows, depth), 1), 8)
    for i in range(4):
        mine = 4 * (12 * core + iota((rows, OC), 0) // 8) + i
        ef = dot_nt((iota((rows, OC), 1) == mine).astype(BF), f).astype(BF)
        e2 = (iota((OC, depth), 0) == 4 * group + ((i - shift) & 3)).astype(BF)
        left[rows * i : rows * (i + 1), :] = jnp.where(diag, dot(ef, e2), 0.0).astype(BF)
    lane = iota((rows, 256), 1) & 127
    for p in range(2):
        for b in range(2):
            for h, ref in enumerate((zb, zo)):
                for q in range(4):
                    slot = slot_of(q, me)
                    for u in range(3):
                        at = 12 * h + 3 * q + u
                        piece = ref[
                            slot, p, 16 * b : 16 * (b + 1), GRP * u : GRP * (u + 1)
                        ].astype(F32)
                        stack[0, 8 * at : 8 * (at + 1), :] = piece[0:8, :]
                        stack[1, 8 * at : 8 * (at + 1), :] = piece[8:16, :]
            for c in range(2):
                wide = stack[c]
                rolled[c, 0:half, :] = wide.astype(BF)
                own[rows * c : rows * (c + 1), :] = wide[0:rows, :].astype(BF)
                for s in range(1, 4):
                    rolled[c, half * s : half * (s + 1), :] = pltpu.roll(wide, OC * s, 1).astype(BF)
            second = dot(own[...], bd)
            for tile in range(3):
                lo, hi = 128 * tile, 128 * (tile + 1)
                rhs = jnp.concatenate([rolled[0, :, lo:hi], rolled[1, :, lo:hi]], axis=1)
                y = dot(left[rows * tile : rows * (tile + 2), :], rhs)
                v = jnp.where(lane < 96 - 32 * tile, y[0:rows, :], y[rows:, :])
                for c in range(2):
                    w = v[:, 128 * c : 128 * (c + 1)] + second[rows * c : rows * (c + 1), lo:hi]
                    for g in range(12):
                        q, u = divmod(g, 3)
                        oo[
                            q,
                            p,
                            16 * b + 8 * c : 16 * b + 8 * (c + 1),
                            GRP * u + lo : GRP * u + hi,
                        ] = w[8 * g : 8 * (g + 1), :]


def mm_kernel(fock, x, out):
    n = NV * VP
    count = NV * VL
    row = iota((n, count), 0)
    pick = (VL * (row // VP) + lax.rem(row, VP) == iota((n, count), 1)) & (lax.rem(row, VP) < VL)
    pick = pick.astype(BF)
    padded = dot_nt(dot(pick, fock[...]).astype(BF), pick).astype(BF)
    y = dot(padded, x[...].reshape(n, COLS)).astype(BF)
    out[...] = y.reshape(NV, VP, COLS)


def gather_kernel(ids, after, *refs):
    me, out = ids[0], refs[4]
    del after
    for t in range(4):
        at = 2 * lax.rem(me - t + Z, 4)
        for p in range(2):
            out[at + p] = refs[t][p]


def singles_of(ref):
    mask = iota((16, 128), 0) == SPARE - 16
    rows = []
    for r in range(Z):
        x = ref[r, 16:32, 0:128].astype(F32)
        rows.append(jnp.sum(jnp.where(mask, x, 0.0), axis=0, keepdims=True))
    return jnp.concatenate(rows, axis=0)


def outer_kernel(ids, mine, theirs, w, out_mine, out_theirs):
    core, k = ids[1], 16 * KH
    t1 = jnp.concatenate([singles_of(mine), singles_of(theirs)], axis=0).astype(BF)
    e1 = (iota((256, 16), 0) // 16 == iota((256, 16), 1)).astype(BF)
    e2 = (iota((128, k), 0) == KH * core + lax.rem(iota((128, k), 1), KH)).astype(BF)
    spread = dot(dot(e1, t1).astype(BF), e2)
    diag = lax.rem(iota((256, k), 0), 16) == iota((256, k), 1) // KH
    spread = jnp.where(diag, -spread, 0.0).astype(BF)
    for b, (first, last) in enumerate(((0, 16), (16, VL))):
        depth = (last - first) * KH
        y = dot(spread[:, 0:depth], w[first:last].reshape(depth, BLK)).astype(BF)
        for n in range(Z):
            out_mine[n, 16 * b : 16 * (b + 1), :] = y[16 * n : 16 * (n + 1), :]
            out_theirs[n, 16 * b : 16 * (b + 1), :] = y[128 + 16 * n : 128 + 16 * (n + 1), :]


def add_kernel(ids, a, b, out):
    me = ids[0]
    for t in range(4):
        at = 2 * lax.rem(me - t + Z, 4)
        for p in range(2):
            out[t, p] = (a[at + p].astype(F32) + b[at + p].astype(F32)).astype(BF)


def coupling_kernel(mine, theirs, w, out, t):
    for b in range(2):
        for j, ref in enumerate((mine, theirs)):
            t[b, 128 * j : 128 * (j + 1), :] = ref[:, 16 * b : 16 * (b + 1), :].reshape(128, BLK)
    total = jnp.zeros((KH, 256), F32)
    for b, (first, last) in enumerate(((0, 16), (16, VL))):
        depth = (last - first) * KH
        g = dot_nt(w[first:last].reshape(depth, BLK), t[b])
        g = jnp.where(iota(g.shape, 0) // KH == lax.rem(iota(g.shape, 1), 16), g, 0.0)
        total += jnp.sum(g.reshape(last - first, KH, 256), axis=0)
    right = (iota((256, 16), 0) // 16 == iota((256, 16), 1)).astype(F32)
    out[...] = dot(total, right, HI)


def x_kernel(ids, after, vv, oo, x, keep, send):
    core = ids[1]
    del after

    def work(own):
        for p in range(2):
            out = keep if p == own else send
            for q in range(4):
                for g, a, b, lo, hi in tiles_of(36 * p + 9 * q, 9):
                    v = vv[g, :, a:b].astype(F32) - oo[q, p, :, lo:hi]
                    x[q, p, :, lo:hi] = v
                    out[q, :, lo:hi] = v.astype(BF)
                out[q, VL:VP, :] = jnp.zeros((VP - VL, BLK), BF)

    pl.when(core == 0)(lambda: work(0))
    pl.when(core == 1)(lambda: work(1))


def merge_kernel(ids, keep, recv, out):
    core = ids[1]
    out[pl.ds(4 * core, 4)] = keep[...]
    out[pl.ds(4 - 4 * core, 4)] = recv[...]


def products(mine, theirs, y, place):
    scale = 1.0 / math.sqrt(OC * OC * NV * VL)
    same = lax.rem(iota((128, 128), 0), 16) == lax.rem(iota((128, 128), 1), 16)
    left = (iota((Z, 128), 1) // 16 == iota((Z, 128), 0)).astype(F32)
    rows = []
    for ref in (mine, theirs):
        g = jnp.zeros((128, 128), F32)
        for b in range(2):
            lhs = ref[:, 16 * b : 16 * (b + 1), :].reshape(128, BLK)
            g += dot_nt(lhs, y[:, 16 * b : 16 * (b + 1), :].reshape(128, BLK))
        rows.append(dot(dot(left, jnp.where(same, g, 0.0), HI), place * scale, HI))
    return rows


def base_kernel(ids, mine, theirs, ov, coupling, rows, t1_out, y):
    me, core = ids[0], ids[1]
    half = (iota((128, KH), 0) == KH * core + iota((128, KH), 1)).astype(F32)
    place_c = (iota((KH, 128), 1) == KH * core + iota((KH, 128), 0)).astype(F32)
    near, far = 8 * core, 8 - 8 * core
    n16 = iota((16, 128), 0)
    place = (iota((16, 128), 1) == OC + jnp.where(n16 < 8, n16 + near, n16 - near)).astype(F32)
    c = coupling[...]
    t1 = [singles_of(mine), singles_of(theirs)]
    row = lax.dot_general(
        c, place_c, (((0,), (0,)), ((), ())), preferred_element_type=F32, precision=HI
    )
    both = jnp.concatenate(t1, axis=0)
    row += dot(dot(dot(both, half, HI), c, HI) * (-0.5 / math.sqrt(OC)), place, HI)
    for t in range(4):
        at = 2 * lax.rem(me - t + Z, 4)
        for p in range(2):
            y[at + p] = ov[t, p]
    spot = iota((128, 128), 1) == OC + near + iota((128, 128), 0) // 16
    parts = products(mine, theirs, y, spot.astype(F32))
    rows[...] = row + jnp.concatenate(parts, axis=0)
    for j, start in enumerate((near, far)):
        t1_out[pl.ds(pl.multiple_of(start, 8), 8), :] = t1[j]


def s_kernel(ids, mine, theirs, x, rows, out):
    core = ids[1]
    near, far = 8 * core, 8 - 8 * core
    spot = iota((128, 128), 1) == OC + core + 2 * (iota((128, 128), 0) // 16)
    parts = products(mine, theirs, x, spot.astype(F32))
    for j in range(2):
        row = rows[8 * j : 8 * (j + 1), :] + parts[j]
        start = (near if j == 0 else far) // 2
        for i in range(4):
            pair = jnp.concatenate([row[2 * i : 2 * i + 1, :], row[2 * i + 1 : 2 * i + 2, :]], axis=1)
            out[start + i] = jnp.broadcast_to(pair[None], (2, 1, 256))


def sum_kernel(x, out):
    out[...] = jnp.broadcast_to(jnp.sum(x[...], axis=0, keepdims=True), out.shape)


def final_kernel(ids, conv, active, x, t1, fock, singles, subspace):
    me = ids[0]
    summed = jnp.sum(x[...], axis=0)
    total = jnp.concatenate([summed[:, 0:128], summed[:, 128:256]], axis=0)
    mine = jnp.concatenate([t1[pl.ds(2 * me, 1), :], t1[pl.ds(2 * me + 1, 1), :]], axis=0)[:, 0:OC]
    all_fock = dot(t1[:, 0:OC].astype(BF), fock[...])
    own_fock = dot(mine.astype(BF), fock[...])
    a0 = (1 - conv[2 * me]).astype(F32)
    a1 = (1 - conv[2 * me + 1]).astype(F32)
    own_active = jnp.where(iota((2, OC), 0) == 0, a0, a1)
    singles[...] = own_active * (-own_fock - 0.5 * total[:, 0:OC])
    part = total[:, OC : OC + 2 * Z] - dot_nt(mine, all_fock, HI) * (1.0 / math.sqrt(OC))
    subspace[...] = part * active[...]


def out_kernel(ids, conv, x, *refs):
    me = ids[0]
    out, ov = refs[4], refs[5]
    for t in range(4):
        ov[lax.rem(me + t, 4)] = refs[t][...]
    for p in range(2):
        a = (1 - conv[2 * me + p]).astype(F32)
        for q in range(4):
            v = a * (x[q, p, 0:VL, :] + ov[q, p, 0:VL, :].astype(F32))
            out[p, :, BLK * q : BLK * (q + 1)] = v.astype(BF)


def local(trial_singles, trial_doubles, occ_fock, virt_fock, w_ovoo, w_ooov, converged):
    ids = jnp.stack([lax.axis_index("root"), lax.axis_index("occ")]).astype(jnp.int32)
    active = (1 - converged).astype(F32)[None, :]
    chunks = (4, 2, VP, BLK)
    roots = (Z, VP, BLK)
    w_ovoo = jnp.transpose(w_ovoo, (1, 0, 2))
    w_ooov = jnp.transpose(w_ooov, (1, 0, 2))

    zb, xb = call(
        prep_kernel, (shape(chunks, BF), shape((NV, VP, COLS), BF)), [SMEM, VMEM, VMEM]
    )(ids, trial_doubles, trial_singles)

    gathered = exchange(xb, VIRT)
    blocks = z_steps(zb)
    oo = call(
        oo_kernel,
        shape(chunks, F32),
        [SMEM, VMEM, VMEM, VMEM],
        [
            VMEM((384, 768), BF),
            VMEM((192, GRP), BF),
            VMEM((2, 192, GRP), F32),
            VMEM((2, 768, GRP), BF),
        ],
        flops=2 << 30,
    )(ids, zb, other_core(zb), occ_fock)
    product = call(
        mm_kernel, shape((NV, VP, COLS), BF), [VMEM, VMEM], flops=1 << 29
    )(virt_fock, gathered)
    vv = exchange(product, VIRT)

    mine = call(gather_kernel, shape(roots, BF), [SMEM, pl.ANY] + [VMEM] * 4)(ids, product, *blocks)
    theirs = other_core(mine)
    outer_mine, outer_theirs = call(
        outer_kernel, (shape(roots, BF), shape(roots, BF)), [SMEM, VMEM, VMEM, VMEM], flops=1 << 30
    )(ids, mine, theirs, w_ovoo)
    outer_recv = other_core(outer_theirs)
    ov = call(add_kernel, shape(chunks, BF), [SMEM, VMEM, VMEM])(ids, outer_mine, outer_recv)
    ov_owned = z_steps(ov, back=True)
    coupling = call(
        coupling_kernel,
        shape((KH, 16), F32),
        [VMEM, VMEM, VMEM],
        [VMEM((2, 256, BLK), BF)],
        flops=1 << 30,
    )(mine, theirs, w_ooov)

    half = (4, VP, BLK)
    x, keep, send = call(
        x_kernel, (shape(chunks, F32), shape(half, BF), shape(half, BF)), [SMEM, pl.ANY, VMEM, VMEM]
    )(ids, coupling, vv, oo)
    recv = other_core(send)
    x_root = call(merge_kernel, shape(roots, BF), [SMEM, VMEM, VMEM])(
        ids, keep, recv
    )
    x_blocks = exchange(x_root, "root")
    rows, t1 = call(
        base_kernel,
        (shape((16, 128), F32), shape((16, 128), F32)),
        [SMEM, VMEM, VMEM, VMEM, VMEM],
        [VMEM(roots, BF)],
    )(ids, mine, theirs, ov, coupling)
    message = call(
        s_kernel, shape((Z, 2, 1, 256), F32), [SMEM, VMEM, VMEM, VMEM, VMEM]
    )(ids, mine, theirs, x_blocks, rows)
    arrived = exchange(message.reshape(16, 1, 256), ROOT_OCC)
    copies = call(sum_kernel, shape((NV, 1, 256), F32), [VMEM])(arrived)
    arrived = exchange(copies, VIRT)
    sigma_singles, subspace = call(
        final_kernel,
        (shape((2, OC), F32), shape((2, 2 * Z), F32)),
        [SMEM, SMEM, VMEM, VMEM, VMEM, VMEM],
    )(ids, converged, active, arrived, t1, occ_fock)

    sigma_doubles = call(
        out_kernel, shape((2, VL, HALF), BF), [SMEM, SMEM] + [VMEM] * 5, [VMEM(chunks, BF)]
    )(ids, converged, x, *ov_owned)
    return (sigma_doubles, sigma_singles, subspace)


def solution(mesh):
    torus = Mesh(
        mesh.devices.reshape(mesh.shape["root"], 4, 4, mesh.shape["occ"]),
        ("root", "virt_0", "virt_1", "occ"),
    )
    return jax.shard_map(
        local,
        mesh=torus,
        in_specs=(
            P("root", None),
            P("root", VIRT, "occ"),
            P(),
            P(),
            P("occ", VIRT, "root"),
            P("occ", VIRT, "root"),
            P(),
        ),
        out_specs=(P("root", VIRT, "occ"), P("root", None), P("root", None)),
        check_vma=False,
    )
```

```python
import math

import jax
import jax.numpy as jnp
from jax import lax
from jax.experimental import pallas as pl
from jax.experimental.pallas import tpu as pltpu
from jax.sharding import Mesh
from jax.sharding import PartitionSpec as P


VIRT = ("virt_0", "virt_1")
ROOT_OCC = ("root", "occ")
BF = jnp.bfloat16
F32 = jnp.float32
HI = lax.Precision.HIGHEST

Z = 8
NV = 16
OC = 96
VL = 30
VP = 32
BLK = 1152
HALF = 4608
COLS = 640
KH = 48
SPARE = 30
GRP = 384

VMEM = pltpu.VMEM
SMEM = pltpu.SMEM


def iota(shape, dim):
    return lax.broadcasted_iota(jnp.int32, shape, dim)


def dot(a, b, precision=None):
    return jnp.dot(a, b, preferred_element_type=F32, precision=precision)


def dot_nt(a, b, precision=None):
    return lax.dot_general(
        a, b, (((1,), (1,)), ((), ())), preferred_element_type=F32, precision=precision
    )


def call(kernel, outs, places, scratch=(), limit=12, flops=1 << 24):
    return pl.pallas_call(
        kernel,
        out_shape=outs,
        in_specs=[pl.BlockSpec(memory_space=p) for p in places],
        out_specs=jax.tree.map(lambda _: pl.BlockSpec(memory_space=VMEM), outs),
        scratch_shapes=scratch,
        compiler_params=pltpu.CompilerParams(vmem_limit_bytes=limit << 20),
        cost_estimate=pl.CostEstimate(flops=flops, bytes_accessed=1 << 20, transcendentals=0),
    )


def exchange(x, axes):
    return lax.all_to_all(x, axes, split_axis=0, concat_axis=0, tiled=True)


def shape(dims, dtype):
    return jax.ShapeDtypeStruct(dims, dtype)


def other_core(x):
    return lax.ppermute(x, "occ", [(0, 1), (1, 0)])


def z_pairs(t):
    return [
        (2 * r + o, 2 * (4 * o + (r + t) % 4) + r // 4) for r in range(Z) for o in range(2)
    ]


def z_steps(x, back=False):
    out = []
    for t in range(4):
        pairs = [(b, a) if back else (a, b) for a, b in z_pairs(t)]
        out.append(lax.ppermute(x[t], ROOT_OCC, pairs))
    return out


def slot_of(q, me):
    return lax.rem(q - me + Z, 4)


def tiles_of(first, count):
    tile, out = 0, []
    while tile < count:
        g, off = divmod(first + tile, 5)
        n = min(5 - off, count - tile)
        out.append((g, 128 * off, 128 * (off + n), 128 * tile, 128 * (tile + n)))
        tile += n
    return out


def prep_kernel(ids, doubles, t1, zb, xb):
    me = ids[0]
    place = (iota((OC, 128), 0) == iota((OC, 128), 1)).astype(F32)
    wide = dot(t1[...].astype(F32), place, HI)
    first = iota((2, 128), 0) == 0
    xb[:, VL:VP, :] = jnp.zeros((NV, VP - VL, COLS), BF)
    xb[14, 0:VL, 256:COLS] = jnp.zeros((VL, COLS - 256), BF)
    xb[15, 0:VL, :] = jnp.zeros((VL, COLS), BF)
    for p in range(2):
        tail = jnp.where(first, jnp.broadcast_to(wide[p : p + 1, :], (2, 128)), 0.0).astype(BF)
        for q in range(4):
            slot = slot_of(q, me)
            zb[slot, p, 0:VL, :] = doubles[p, :, BLK * q : BLK * (q + 1)]
            zb[slot, p, VL:VP, 0:128] = tail
            zb[slot, p, VL:VP, 128:BLK] = jnp.zeros((VP - VL, BLK - 128), BF)
        for g, a, b, lo, hi in tiles_of(36 * p, 36):
            xb[g, 0:VL, a:b] = doubles[p, :, lo:hi]


def oo_kernel(ids, zb, zo, fock, oo, left, own, stack, rolled):
    me, core = ids[0], ids[1]
    f = fock[...]
    rows, depth, half = 96, 768, 192
    e3 = (lax.rem(iota((GRP, OC), 0), OC) == iota((GRP, OC), 1)).astype(BF)
    same = iota((GRP, GRP), 0) // OC == iota((GRP, GRP), 1) // OC
    bd = dot_nt(dot(e3, f).astype(BF), e3)
    bd = jnp.where(same, bd, 0.0).astype(BF)
    col = iota((OC, depth), 1)
    shift = col // half
    group = lax.rem(col, half) // 8
    group = jnp.where(group < 12, group + 12 * core, group - 12 * core)
    diag = lax.rem(iota((rows, depth), 0), 8) == lax.rem(iota((rows, depth), 1), 8)
    for i in range(4):
        mine = 4 * (12 * core + iota((rows, OC), 0) // 8) + i
        ef = dot_nt((iota((rows, OC), 1) == mine).astype(BF), f).astype(BF)
        e2 = (iota((OC, depth), 0) == 4 * group + ((i - shift) & 3)).astype(BF)
        left[rows * i : rows * (i + 1), :] = jnp.where(diag, dot(ef, e2), 0.0).astype(BF)
    lane = iota((rows, 256), 1) & 127
    for p in range(2):
        for b in range(2):
            for h, ref in enumerate((zb, zo)):
                for q in range(4):
                    slot = slot_of(q, me)
                    for u in range(3):
                        at = 12 * h + 3 * q + u
                        piece = ref[
                            slot, p, 16 * b : 16 * (b + 1), GRP * u : GRP * (u + 1)
                        ].astype(F32)
                        stack[0, 8 * at : 8 * (at + 1), :] = piece[0:8, :]
                        stack[1, 8 * at : 8 * (at + 1), :] = piece[8:16, :]
            for c in range(2):
                wide = stack[c]
                rolled[c, 0:half, :] = wide.astype(BF)
                own[rows * c : rows * (c + 1), :] = wide[0:rows, :].astype(BF)
                for s in range(1, 4):
                    rolled[c, half * s : half * (s + 1), :] = pltpu.roll(wide, OC * s, 1).astype(BF)
            second = dot(own[...], bd)
            for tile in range(3):
                lo, hi = 128 * tile, 128 * (tile + 1)
                rhs = jnp.concatenate([rolled[0, :, lo:hi], rolled[1, :, lo:hi]], axis=1)
                y = dot(left[rows * tile : rows * (tile + 2), :], rhs)
                v = jnp.where(lane < 96 - 32 * tile, y[0:rows, :], y[rows:, :])
                for c in range(2):
                    w = v[:, 128 * c : 128 * (c + 1)] + second[rows * c : rows * (c + 1), lo:hi]
                    for g in range(12):
                        q, u = divmod(g, 3)
                        oo[
                            q,
                            p,
                            16 * b + 8 * c : 16 * b + 8 * (c + 1),
                            GRP * u + lo : GRP * u + hi,
                        ] = w[8 * g : 8 * (g + 1), :]


def mm_kernel(fock, x, out):
    n = NV * VP
    count = NV * VL
    row = iota((n, count), 0)
    pick = (VL * (row // VP) + lax.rem(row, VP) == iota((n, count), 1)) & (lax.rem(row, VP) < VL)
    pick = pick.astype(BF)
    padded = dot_nt(dot(pick, fock[...]).astype(BF), pick).astype(BF)
    y = dot(padded, x[...].reshape(n, COLS)).astype(BF)
    out[...] = y.reshape(NV, VP, COLS)


def gather_kernel(ids, after, *refs):
    me, out = ids[0], refs[4]
    del after
    for t in range(4):
        at = 2 * lax.rem(me - t + Z, 4)
        for p in range(2):
            out[at + p] = refs[t][p]


def singles_of(ref):
    mask = iota((16, 128), 0) == SPARE - 16
    rows = []
    for r in range(Z):
        x = ref[r, 16:32, 0:128].astype(F32)
        rows.append(jnp.sum(jnp.where(mask, x, 0.0), axis=0, keepdims=True))
    return jnp.concatenate(rows, axis=0)


def outer_kernel(ids, mine, theirs, w, out_mine, out_theirs):
    core, k = ids[1], 16 * KH
    t1 = jnp.concatenate([singles_of(mine), singles_of(theirs)], axis=0).astype(BF)
    e1 = (iota((256, 16), 0) // 16 == iota((256, 16), 1)).astype(BF)
    e2 = (iota((128, k), 0) == KH * core + lax.rem(iota((128, k), 1), KH)).astype(BF)
    spread = dot(dot(e1, t1).astype(BF), e2)
    diag = lax.rem(iota((256, k), 0), 16) == iota((256, k), 1) // KH
    spread = jnp.where(diag, -spread, 0.0).astype(BF)
    for b, (first, last) in enumerate(((0, 16), (16, VL))):
        depth = (last - first) * KH
        y = dot(spread[:, 0:depth], w[first:last].reshape(depth, BLK)).astype(BF)
        for n in range(Z):
            out_mine[n, 16 * b : 16 * (b + 1), :] = y[16 * n : 16 * (n + 1), :]
            out_theirs[n, 16 * b : 16 * (b + 1), :] = y[128 + 16 * n : 128 + 16 * (n + 1), :]


def add_kernel(ids, a, b, out):
    me = ids[0]
    for t in range(4):
        at = 2 * lax.rem(me - t + Z, 4)
        for p in range(2):
            out[t, p] = (a[at + p].astype(F32) + b[at + p].astype(F32)).astype(BF)


def coupling_kernel(mine, theirs, w, out, t):
    for b in range(2):
        for j, ref in enumerate((mine, theirs)):
            t[b, 128 * j : 128 * (j + 1), :] = ref[:, 16 * b : 16 * (b + 1), :].reshape(128, BLK)
    total = jnp.zeros((KH, 256), F32)
    for b, (first, last) in enumerate(((0, 16), (16, VL))):
        depth = (last - first) * KH
        g = dot_nt(w[first:last].reshape(depth, BLK), t[b])
        g = jnp.where(iota(g.shape, 0) // KH == lax.rem(iota(g.shape, 1), 16), g, 0.0)
        total += jnp.sum(g.reshape(last - first, KH, 256), axis=0)
    right = (iota((256, 16), 0) // 16 == iota((256, 16), 1)).astype(F32)
    out[...] = dot(total, right, HI)


def x_kernel(ids, after, vv, oo, x, full, send):
    core = ids[1]
    del after

    def work(own):
        for p in range(2):
            for q in range(4):
                out = full.at[4 * own + q] if p == own else send.at[q]
                for g, a, b, lo, hi in tiles_of(36 * p + 9 * q, 9):
                    v = vv[g, :, a:b].astype(F32) - oo[q, p, :, lo:hi]
                    x[q, p, :, lo:hi] = v
                    out[:, lo:hi] = v.astype(BF)
                out[VL:VP, :] = jnp.zeros((VP - VL, BLK), BF)

    pl.when(core == 0)(lambda: work(0))
    pl.when(core == 1)(lambda: work(1))


def products(mine, theirs, y, place):
    scale = 1.0 / math.sqrt(OC * OC * NV * VL)
    same = lax.rem(iota((128, 128), 0), 16) == lax.rem(iota((128, 128), 1), 16)
    left = (iota((Z, 128), 1) // 16 == iota((Z, 128), 0)).astype(F32)
    rows = []
    for ref in (mine, theirs):
        g = jnp.zeros((128, 128), F32)
        for b in range(2):
            lhs = ref[:, 16 * b : 16 * (b + 1), :].reshape(128, BLK)
            g += dot_nt(lhs, y[:, 16 * b : 16 * (b + 1), :].reshape(128, BLK))
        rows.append(dot(dot(left, jnp.where(same, g, 0.0), HI), place * scale, HI))
    return rows


def base_kernel(ids, mine, theirs, ov, coupling, fock, rows, singles_out, sub_out, y, t1_all):
    me, core = ids[0], ids[1]
    half = (iota((128, KH), 0) == KH * core + iota((128, KH), 1)).astype(F32)
    place_c = (iota((KH, 128), 1) == KH * core + iota((KH, 128), 0)).astype(F32)
    near, far = 8 * core, 8 - 8 * core
    n16 = iota((16, 128), 0)
    place = (iota((16, 128), 1) == OC + jnp.where(n16 < 8, n16 + near, n16 - near)).astype(F32)
    c = coupling[...]
    t1 = [singles_of(mine), singles_of(theirs)]
    row = lax.dot_general(
        c, place_c, (((0,), (0,)), ((), ())), preferred_element_type=F32, precision=HI
    )
    both = jnp.concatenate(t1, axis=0)
    row += dot(dot(dot(both, half, HI), c, HI) * (-0.5 / math.sqrt(OC)), place, HI)
    for t in range(4):
        at = 2 * lax.rem(me - t + Z, 4)
        for p in range(2):
            y[at + p] = ov[t, p]
    spot = iota((128, 128), 1) == OC + near + iota((128, 128), 0) // 16
    parts = products(mine, theirs, y, spot.astype(F32))
    rows[...] = row + jnp.concatenate(parts, axis=0)
    for j, start in enumerate((near, far)):
        t1_all[pl.ds(pl.multiple_of(start, 8), 8), :] = t1[j]
    own = [t1_all[pl.ds(2 * me + p, 1), :] for p in range(2)]
    own = jnp.concatenate(own, axis=0)[:, 0:OC]
    all_fock = dot(t1_all[:, 0:OC].astype(BF), fock[...])
    singles_out[...] = -dot(own.astype(BF), fock[...])
    sub_out[...] = -dot_nt(own, all_fock, HI) * (1.0 / math.sqrt(OC))


def s_kernel(ids, mine, theirs, x, rows, out):
    core = ids[1]
    near, far = 8 * core, 8 - 8 * core
    spot = iota((128, 128), 1) == OC + core + 2 * (iota((128, 128), 0) // 16)
    parts = products(mine, theirs, x, spot.astype(F32))
    for j in range(2):
        row = rows[8 * j : 8 * (j + 1), :] + parts[j]
        start = (near if j == 0 else far) // 2
        for i in range(4):
            pair = jnp.concatenate([row[2 * i : 2 * i + 1, :], row[2 * i + 1 : 2 * i + 2, :]], axis=1)
            out[start + i] = jnp.broadcast_to(pair[None], (2, 1, 256))


def sum_kernel(x, out):
    out[...] = jnp.broadcast_to(jnp.sum(x[...], axis=0, keepdims=True), out.shape)


def final_kernel(ids, conv, active, x, own_singles, own_sub, singles, subspace):
    me = ids[0]
    summed = jnp.sum(x[...], axis=0)
    total = jnp.concatenate([summed[:, 0:128], summed[:, 128:256]], axis=0)
    a0 = (1 - conv[2 * me]).astype(F32)
    a1 = (1 - conv[2 * me + 1]).astype(F32)
    own_active = jnp.where(iota((2, OC), 0) == 0, a0, a1)
    singles[...] = own_active * (own_singles[...] - 0.5 * total[:, 0:OC])
    subspace[...] = (total[:, OC : OC + 2 * Z] + own_sub[...]) * active[...]


def out_kernel(ids, conv, x, *refs):
    me = ids[0]
    out, ov = refs[4], refs[5]
    for t in range(4):
        ov[lax.rem(me + t, 4)] = refs[t][...]
    for p in range(2):
        a = (1 - conv[2 * me + p]).astype(F32)
        for q in range(4):
            v = a * (x[q, p, 0:VL, :] + ov[q, p, 0:VL, :].astype(F32))
            out[p, :, BLK * q : BLK * (q + 1)] = v.astype(BF)


def local(trial_singles, trial_doubles, occ_fock, virt_fock, w_ovoo, w_ooov, converged):
    ids = jnp.stack([lax.axis_index("root"), lax.axis_index("occ")]).astype(jnp.int32)
    active = (1 - converged).astype(F32)[None, :]
    chunks = (4, 2, VP, BLK)
    roots = (Z, VP, BLK)
    w_ovoo = jnp.transpose(w_ovoo, (1, 0, 2))
    w_ooov = jnp.transpose(w_ooov, (1, 0, 2))

    zb, xb = call(
        prep_kernel, (shape(chunks, BF), shape((NV, VP, COLS), BF)), [SMEM, VMEM, VMEM]
    )(ids, trial_doubles, trial_singles)

    gathered = exchange(xb, VIRT)
    blocks = z_steps(zb)
    oo = call(
        oo_kernel,
        shape(chunks, F32),
        [SMEM, VMEM, VMEM, VMEM],
        [
            VMEM((384, 768), BF),
            VMEM((192, GRP), BF),
            VMEM((2, 192, GRP), F32),
            VMEM((2, 768, GRP), BF),
        ],
        flops=2 << 30,
    )(ids, zb, other_core(zb), occ_fock)
    product = call(
        mm_kernel, shape((NV, VP, COLS), BF), [VMEM, VMEM], flops=1 << 29
    )(virt_fock, gathered)
    vv = exchange(product, VIRT)

    mine = call(gather_kernel, shape(roots, BF), [SMEM, pl.ANY] + [VMEM] * 4)(ids, product, *blocks)
    theirs = other_core(mine)
    outer_mine, outer_theirs = call(
        outer_kernel, (shape(roots, BF), shape(roots, BF)), [SMEM, VMEM, VMEM, VMEM], flops=1 << 30
    )(ids, mine, theirs, w_ovoo)
    outer_recv = other_core(outer_theirs)
    ov = call(add_kernel, shape(chunks, BF), [SMEM, VMEM, VMEM])(ids, outer_mine, outer_recv)
    ov_owned = z_steps(ov, back=True)
    coupling = call(
        coupling_kernel,
        shape((KH, 16), F32),
        [VMEM, VMEM, VMEM],
        [VMEM((2, 256, BLK), BF)],
        flops=1 << 30,
    )(mine, theirs, w_ooov)

    x, full, send = call(
        x_kernel,
        (shape(chunks, F32), shape(roots, BF), shape((4, VP, BLK), BF)),
        [SMEM, pl.ANY, VMEM, VMEM],
    )(ids, coupling, vv, oo)
    recv = other_core(send)
    other = 4 * (1 - lax.axis_index("occ"))
    x_root = lax.dynamic_update_slice_in_dim(full, recv, other, 0)
    x_blocks = exchange(x_root, "root")
    rows, own_singles, own_sub = call(
        base_kernel,
        (shape((16, 128), F32), shape((2, OC), F32), shape((2, 2 * Z), F32)),
        [SMEM] + [VMEM] * 5,
        [VMEM(roots, BF), VMEM((16, 128), F32)],
    )(ids, mine, theirs, ov, coupling, occ_fock)
    message = call(
        s_kernel, shape((Z, 2, 1, 256), F32), [SMEM, VMEM, VMEM, VMEM, VMEM]
    )(ids, mine, theirs, x_blocks, rows)
    arrived = exchange(message.reshape(16, 1, 256), ROOT_OCC)
    copies = call(sum_kernel, shape((NV, 1, 256), F32), [VMEM])(arrived)
    arrived = exchange(copies, VIRT)
    sigma_singles, subspace = call(
        final_kernel,
        (shape((2, OC), F32), shape((2, 2 * Z), F32)),
        [SMEM, SMEM, VMEM, VMEM, VMEM, VMEM],
    )(ids, converged, active, arrived, own_singles, own_sub)

    sigma_doubles = call(
        out_kernel, shape((2, VL, HALF), BF), [SMEM, SMEM] + [VMEM] * 5, [VMEM(chunks, BF)]
    )(ids, converged, x, *ov_owned)
    return (sigma_doubles, sigma_singles, subspace)


def solution(mesh):
    torus = Mesh(
        mesh.devices.reshape(mesh.shape["root"], 4, 4, mesh.shape["occ"]),
        ("root", "virt_0", "virt_1", "occ"),
    )
    return jax.shard_map(
        local,
        mesh=torus,
        in_specs=(
            P("root", None),
            P("root", VIRT, "occ"),
            P(),
            P(),
            P("occ", VIRT, "root"),
            P("occ", VIRT, "root"),
            P(),
        ),
        out_specs=(P("root", VIRT, "occ"), P("root", None), P("root", None)),
        check_vma=False,
    )
```

```python
import math

import jax
import jax.numpy as jnp
from jax import lax
from jax.experimental import pallas as pl
from jax.experimental.pallas import tpu as pltpu
from jax.sharding import Mesh
from jax.sharding import PartitionSpec as P


VIRT = ("virt_0", "virt_1")
ROOT_OCC = ("root", "occ")
BF = jnp.bfloat16
F32 = jnp.float32
HI = lax.Precision.HIGHEST

Z = 8
NV = 16
OC = 96
VL = 30
VP = 32
BLK = 1152
HALF = 4608
COLS = 640
KH = 48
SPARE = 30
GRP = 384

VMEM = pltpu.VMEM
SMEM = pltpu.SMEM


def iota(shape, dim):
    return lax.broadcasted_iota(jnp.int32, shape, dim)


def dot(a, b, precision=None):
    return jnp.dot(a, b, preferred_element_type=F32, precision=precision)


def dot_nt(a, b, precision=None):
    return lax.dot_general(
        a, b, (((1,), (1,)), ((), ())), preferred_element_type=F32, precision=precision
    )


def call(kernel, outs, places, scratch=(), limit=12, flops=1 << 24):
    return pl.pallas_call(
        kernel,
        out_shape=outs,
        in_specs=[pl.BlockSpec(memory_space=p) for p in places],
        out_specs=jax.tree.map(lambda _: pl.BlockSpec(memory_space=VMEM), outs),
        scratch_shapes=scratch,
        compiler_params=pltpu.CompilerParams(vmem_limit_bytes=limit << 20),
        cost_estimate=pl.CostEstimate(flops=flops, bytes_accessed=1 << 20, transcendentals=0),
    )


def exchange(x, axes):
    return lax.all_to_all(x, axes, split_axis=0, concat_axis=0, tiled=True)


def shape(dims, dtype):
    return jax.ShapeDtypeStruct(dims, dtype)


def other_core(x):
    return lax.ppermute(x, "occ", [(0, 1), (1, 0)])


def z_pairs(t):
    return [
        (2 * r + o, 2 * (4 * o + (r + t) % 4) + r // 4) for r in range(Z) for o in range(2)
    ]


def z_steps(x, back=False):
    out = []
    for t in range(4):
        pairs = [(b, a) if back else (a, b) for a, b in z_pairs(t)]
        out.append(lax.ppermute(x[t], ROOT_OCC, pairs))
    return out


def slot_of(q, me):
    return lax.rem(q - me + Z, 4)


def tiles_of(first, count):
    tile, out = 0, []
    while tile < count:
        g, off = divmod(first + tile, 5)
        n = min(5 - off, count - tile)
        out.append((g, 128 * off, 128 * (off + n), 128 * tile, 128 * (tile + n)))
        tile += n
    return out


def prep_kernel(ids, doubles, t1, zb, xb):
    me = ids[0]
    place = (iota((OC, 128), 0) == iota((OC, 128), 1)).astype(F32)
    wide = dot(t1[...].astype(F32), place, HI)
    first = iota((2, 128), 0) == 0
    xb[:, VL:VP, :] = jnp.zeros((NV, VP - VL, COLS), BF)
    xb[14, 0:VL, 256:COLS] = jnp.zeros((VL, COLS - 256), BF)
    xb[15, 0:VL, :] = jnp.zeros((VL, COLS), BF)
    for p in range(2):
        tail = jnp.where(first, jnp.broadcast_to(wide[p : p + 1, :], (2, 128)), 0.0).astype(BF)
        for q in range(4):
            slot = slot_of(q, me)
            zb[slot, p, 0:VL, :] = doubles[p, :, BLK * q : BLK * (q + 1)]
            zb[slot, p, VL:VP, 0:128] = tail
            zb[slot, p, VL:VP, 128:BLK] = jnp.zeros((VP - VL, BLK - 128), BF)
        for g, a, b, lo, hi in tiles_of(36 * p, 36):
            xb[g, 0:VL, a:b] = doubles[p, :, lo:hi]


def oo_kernel(ids, zb, zo, fock, oo, left, own, stack, rolled):
    me, core = ids[0], ids[1]
    f = fock[...]
    rows, depth, half = 96, 768, 192
    e3 = (lax.rem(iota((GRP, OC), 0), OC) == iota((GRP, OC), 1)).astype(BF)
    same = iota((GRP, GRP), 0) // OC == iota((GRP, GRP), 1) // OC
    bd = dot_nt(dot(e3, f).astype(BF), e3)
    bd = jnp.where(same, bd, 0.0).astype(BF)
    col = iota((OC, depth), 1)
    shift = col // half
    group = lax.rem(col, half) // 8
    group = jnp.where(group < 12, group + 12 * core, group - 12 * core)
    diag = lax.rem(iota((rows, depth), 0), 8) == lax.rem(iota((rows, depth), 1), 8)
    for i in range(4):
        mine = 4 * (12 * core + iota((rows, OC), 0) // 8) + i
        ef = dot_nt((iota((rows, OC), 1) == mine).astype(BF), f).astype(BF)
        e2 = (iota((OC, depth), 0) == 4 * group + ((i - shift) & 3)).astype(BF)
        left[rows * i : rows * (i + 1), :] = jnp.where(diag, dot(ef, e2), 0.0).astype(BF)
    lane = iota((rows, 256), 1) & 127
    for p in range(2):
        for b in range(2):
            for h, ref in enumerate((zb, zo)):
                for q in range(4):
                    slot = slot_of(q, me)
                    for u in range(3):
                        at = 12 * h + 3 * q + u
                        piece = ref[
                            slot, p, 16 * b : 16 * (b + 1), GRP * u : GRP * (u + 1)
                        ].astype(F32)
                        stack[0, 8 * at : 8 * (at + 1), :] = piece[0:8, :]
                        stack[1, 8 * at : 8 * (at + 1), :] = piece[8:16, :]
            for c in range(2):
                wide = stack[c]
                rolled[c, 0:half, :] = wide.astype(BF)
                own[rows * c : rows * (c + 1), :] = wide[0:rows, :].astype(BF)
                for s in range(1, 4):
                    rolled[c, half * s : half * (s + 1), :] = pltpu.roll(wide, OC * s, 1).astype(BF)
            second = dot(own[...], bd)
            for tile in range(3):
                lo, hi = 128 * tile, 128 * (tile + 1)
                rhs = jnp.concatenate([rolled[0, :, lo:hi], rolled[1, :, lo:hi]], axis=1)
                y = dot(left[rows * tile : rows * (tile + 2), :], rhs)
                v = jnp.where(lane < 96 - 32 * tile, y[0:rows, :], y[rows:, :])
                w = [
                    v[:, 128 * c : 128 * (c + 1)] + second[rows * c : rows * (c + 1), lo:hi]
                    for c in range(2)
                ]
                for g in range(12):
                    q, u = divmod(g, 3)
                    part = jnp.concatenate([y[8 * g : 8 * (g + 1), :] for y in w], axis=0)
                    at = GRP * u + lo
                    oo[q, p, 16 * b : 16 * (b + 1), at : at + 128] = part.astype(BF)


def mm_kernel(fock, x, out):
    n = NV * VP
    count = NV * VL
    row = iota((n, count), 0)
    pick = (VL * (row // VP) + lax.rem(row, VP) == iota((n, count), 1)) & (lax.rem(row, VP) < VL)
    pick = pick.astype(BF)
    padded = dot_nt(dot(pick, fock[...]).astype(BF), pick).astype(BF)
    y = dot(padded, x[...].reshape(n, COLS)).astype(BF)
    out[...] = y.reshape(NV, VP, COLS)


def gather_kernel(ids, after, *refs):
    me, out = ids[0], refs[4]
    del after
    for t in range(4):
        at = 2 * lax.rem(me - t + Z, 4)
        for p in range(2):
            out[at + p] = refs[t][p]


def singles_of(ref):
    mask = iota((16, 128), 0) == SPARE - 16
    rows = []
    for r in range(Z):
        x = ref[r, 16:32, 0:128].astype(F32)
        rows.append(jnp.sum(jnp.where(mask, x, 0.0), axis=0, keepdims=True))
    return jnp.concatenate(rows, axis=0)


def outer_kernel(ids, mine, theirs, w, out_mine, out_theirs):
    core, k = ids[1], 16 * KH
    t1 = jnp.concatenate([singles_of(mine), singles_of(theirs)], axis=0).astype(BF)
    e1 = (iota((256, 16), 0) // 16 == iota((256, 16), 1)).astype(BF)
    e2 = (iota((128, k), 0) == KH * core + lax.rem(iota((128, k), 1), KH)).astype(BF)
    spread = dot(dot(e1, t1).astype(BF), e2)
    diag = lax.rem(iota((256, k), 0), 16) == iota((256, k), 1) // KH
    spread = jnp.where(diag, -spread, 0.0).astype(BF)
    for b, (first, last) in enumerate(((0, 16), (16, VL))):
        depth = (last - first) * KH
        y = dot(spread[:, 0:depth], w[first:last].reshape(depth, BLK)).astype(BF)
        for n in range(Z):
            out_mine[n, 16 * b : 16 * (b + 1), :] = y[16 * n : 16 * (n + 1), :]
            out_theirs[n, 16 * b : 16 * (b + 1), :] = y[128 + 16 * n : 128 + 16 * (n + 1), :]


def add_kernel(ids, a, b, out):
    me = ids[0]
    for t in range(4):
        at = 2 * lax.rem(me - t + Z, 4)
        for p in range(2):
            out[t, p] = (a[at + p].astype(F32) + b[at + p].astype(F32)).astype(BF)


def coupling_kernel(mine, theirs, w, out, t):
    for b in range(2):
        for j, ref in enumerate((mine, theirs)):
            t[b, 128 * j : 128 * (j + 1), :] = ref[:, 16 * b : 16 * (b + 1), :].reshape(128, BLK)
    total = jnp.zeros((KH, 256), F32)
    for b, (first, last) in enumerate(((0, 16), (16, VL))):
        depth = (last - first) * KH
        g = dot_nt(w[first:last].reshape(depth, BLK), t[b])
        g = jnp.where(iota(g.shape, 0) // KH == lax.rem(iota(g.shape, 1), 16), g, 0.0)
        total += jnp.sum(g.reshape(last - first, KH, 256), axis=0)
    right = (iota((256, 16), 0) // 16 == iota((256, 16), 1)).astype(F32)
    out[...] = dot(total, right, HI)


def x_kernel(ids, vv, oo, x, keep, send):
    core = ids[1]

    def work(own):
        for p in range(2):
            out = keep if p == own else send
            for q in range(4):
                for g, a, b, lo, hi in tiles_of(36 * p + 9 * q, 9):
                    v = vv[g, :, a:b].astype(F32) - oo[q, p, :, lo:hi].astype(F32)
                    x[q, p, :, lo:hi] = v
                    out[q, :, lo:hi] = v.astype(BF)
                out[q, VL:VP, :] = jnp.zeros((VP - VL, BLK), BF)

    pl.when(core == 0)(lambda: work(0))
    pl.when(core == 1)(lambda: work(1))


def merge_kernel(ids, keep, recv, out):
    core = ids[1]
    out[pl.ds(4 * core, 4)] = keep[...]
    out[pl.ds(4 - 4 * core, 4)] = recv[...]


def products(mine, theirs, y, place):
    scale = 1.0 / math.sqrt(OC * OC * NV * VL)
    same = lax.rem(iota((128, 128), 0), 16) == lax.rem(iota((128, 128), 1), 16)
    left = (iota((Z, 128), 1) // 16 == iota((Z, 128), 0)).astype(F32)
    rows = []
    for ref in (mine, theirs):
        g = jnp.zeros((128, 128), F32)
        for b in range(2):
            lhs = ref[:, 16 * b : 16 * (b + 1), :].reshape(128, BLK)
            g += dot_nt(lhs, y[:, 16 * b : 16 * (b + 1), :].reshape(128, BLK))
        rows.append(dot(dot(left, jnp.where(same, g, 0.0), HI), place * scale, HI))
    return rows


def base_kernel(ids, mine, theirs, ov, coupling, rows, t1_out, y):
    me, core = ids[0], ids[1]
    half = (iota((128, KH), 0) == KH * core + iota((128, KH), 1)).astype(F32)
    place_c = (iota((KH, 128), 1) == KH * core + iota((KH, 128), 0)).astype(F32)
    near, far = 8 * core, 8 - 8 * core
    n16 = iota((16, 128), 0)
    place = (iota((16, 128), 1) == OC + jnp.where(n16 < 8, n16 + near, n16 - near)).astype(F32)
    c = coupling[...]
    t1 = [singles_of(mine), singles_of(theirs)]
    row = lax.dot_general(
        c, place_c, (((0,), (0,)), ((), ())), preferred_element_type=F32, precision=HI
    )
    both = jnp.concatenate(t1, axis=0)
    row += dot(dot(dot(both, half, HI), c, HI) * (-0.5 / math.sqrt(OC)), place, HI)
    for t in range(4):
        at = 2 * lax.rem(me - t + Z, 4)
        for p in range(2):
            y[at + p] = ov[t, p]
    spot = iota((128, 128), 1) == OC + near + iota((128, 128), 0) // 16
    parts = products(mine, theirs, y, spot.astype(F32))
    rows[...] = row + jnp.concatenate(parts, axis=0)
    for j, start in enumerate((near, far)):
        t1_out[pl.ds(pl.multiple_of(start, 8), 8), :] = t1[j]


def s_kernel(ids, mine, theirs, x, rows, out):
    core = ids[1]
    near, far = 8 * core, 8 - 8 * core
    spot = iota((128, 128), 1) == OC + core + 2 * (iota((128, 128), 0) // 16)
    parts = products(mine, theirs, x, spot.astype(F32))
    for j in range(2):
        row = rows[8 * j : 8 * (j + 1), :] + parts[j]
        start = (near if j == 0 else far) // 2
        for i in range(4):
            pair = jnp.concatenate([row[2 * i : 2 * i + 1, :], row[2 * i + 1 : 2 * i + 2, :]], axis=1)
            out[start + i] = jnp.broadcast_to(pair[None], (2, 1, 256))


def sum_kernel(x, out):
    out[...] = jnp.broadcast_to(jnp.sum(x[...], axis=0, keepdims=True), out.shape)


def final_kernel(ids, conv, active, x, t1, fock, singles, subspace):
    me = ids[0]
    summed = jnp.sum(x[...], axis=0)
    total = jnp.concatenate([summed[:, 0:128], summed[:, 128:256]], axis=0)
    mine = jnp.concatenate([t1[pl.ds(2 * me, 1), :], t1[pl.ds(2 * me + 1, 1), :]], axis=0)[:, 0:OC]
    all_fock = dot(t1[:, 0:OC].astype(BF), fock[...])
    own_fock = dot(mine.astype(BF), fock[...])
    a0 = (1 - conv[2 * me]).astype(F32)
    a1 = (1 - conv[2 * me + 1]).astype(F32)
    own_active = jnp.where(iota((2, OC), 0) == 0, a0, a1)
    singles[...] = own_active * (-own_fock - 0.5 * total[:, 0:OC])
    part = total[:, OC : OC + 2 * Z] - dot_nt(mine, all_fock, HI) * (1.0 / math.sqrt(OC))
    subspace[...] = part * active[...]


def out_kernel(ids, conv, x, *refs):
    me = ids[0]
    out, ov = refs[4], refs[5]
    for t in range(4):
        ov[lax.rem(me + t, 4)] = refs[t][...]
    for p in range(2):
        a = (1 - conv[2 * me + p]).astype(F32)
        for q in range(4):
            v = a * (x[q, p, 0:VL, :] + ov[q, p, 0:VL, :].astype(F32))
            out[p, :, BLK * q : BLK * (q + 1)] = v.astype(BF)


def local(trial_singles, trial_doubles, occ_fock, virt_fock, w_ovoo, w_ooov, converged):
    ids = jnp.stack([lax.axis_index("root"), lax.axis_index("occ")]).astype(jnp.int32)
    active = (1 - converged).astype(F32)[None, :]
    chunks = (4, 2, VP, BLK)
    roots = (Z, VP, BLK)
    w_ovoo = jnp.transpose(w_ovoo, (1, 0, 2))
    w_ooov = jnp.transpose(w_ooov, (1, 0, 2))

    zb, xb = call(
        prep_kernel, (shape(chunks, BF), shape((NV, VP, COLS), BF)), [SMEM, VMEM, VMEM]
    )(ids, trial_doubles, trial_singles)

    gathered = exchange(xb, VIRT)
    blocks = z_steps(zb)
    oo = call(
        oo_kernel,
        shape(chunks, BF),
        [SMEM, VMEM, VMEM, VMEM],
        [
            VMEM((384, 768), BF),
            VMEM((192, GRP), BF),
            VMEM((2, 192, GRP), F32),
            VMEM((2, 768, GRP), BF),
        ],
        flops=2 << 30,
    )(ids, zb, other_core(zb), occ_fock)
    product = call(
        mm_kernel, shape((NV, VP, COLS), BF), [VMEM, VMEM], flops=1 << 29
    )(virt_fock, gathered)
    vv = exchange(product, VIRT)

    mine = call(gather_kernel, shape(roots, BF), [SMEM, pl.ANY] + [VMEM] * 4)(ids, product, *blocks)
    theirs = other_core(mine)
    outer_mine, outer_theirs = call(
        outer_kernel, (shape(roots, BF), shape(roots, BF)), [SMEM, VMEM, VMEM, VMEM], flops=1 << 30
    )(ids, mine, theirs, w_ovoo)
    outer_recv = other_core(outer_theirs)
    ov = call(add_kernel, shape(chunks, BF), [SMEM, VMEM, VMEM])(ids, outer_mine, outer_recv)
    ov_owned = z_steps(ov, back=True)
    coupling = call(
        coupling_kernel,
        shape((KH, 16), F32),
        [VMEM, VMEM, VMEM],
        [VMEM((2, 256, BLK), BF)],
        flops=1 << 30,
    )(mine, theirs, w_ooov)

    half = (4, VP, BLK)
    x, keep, send = call(
        x_kernel, (shape(chunks, F32), shape(half, BF), shape(half, BF)), [SMEM, VMEM, VMEM]
    )(ids, vv, oo)
    recv = other_core(send)
    x_root = call(merge_kernel, shape(roots, BF), [SMEM, VMEM, VMEM])(
        ids, keep, recv
    )
    x_blocks = exchange(x_root, "root")
    rows, t1 = call(
        base_kernel,
        (shape((16, 128), F32), shape((16, 128), F32)),
        [SMEM, VMEM, VMEM, VMEM, VMEM],
        [VMEM(roots, BF)],
    )(ids, mine, theirs, ov, coupling)
    message = call(
        s_kernel, shape((Z, 2, 1, 256), F32), [SMEM, VMEM, VMEM, VMEM, VMEM]
    )(ids, mine, theirs, x_blocks, rows)
    arrived = exchange(message.reshape(16, 1, 256), ROOT_OCC)
    copies = call(sum_kernel, shape((NV, 1, 256), F32), [VMEM])(arrived)
    arrived = exchange(copies, VIRT)
    sigma_singles, subspace = call(
        final_kernel,
        (shape((2, OC), F32), shape((2, 2 * Z), F32)),
        [SMEM, SMEM, VMEM, VMEM, VMEM, VMEM],
    )(ids, converged, active, arrived, t1, occ_fock)

    sigma_doubles = call(
        out_kernel, shape((2, VL, HALF), BF), [SMEM, SMEM] + [VMEM] * 5, [VMEM(chunks, BF)]
    )(ids, converged, x, *ov_owned)
    return (sigma_doubles, sigma_singles, subspace)


def solution(mesh):
    torus = Mesh(
        mesh.devices.reshape(mesh.shape["root"], 4, 4, mesh.shape["occ"]),
        ("root", "virt_0", "virt_1", "occ"),
    )
    return jax.shard_map(
        local,
        mesh=torus,
        in_specs=(
            P("root", None),
            P("root", VIRT, "occ"),
            P(),
            P(),
            P("occ", VIRT, "root"),
            P("occ", VIRT, "root"),
            P(),
        ),
        out_specs=(P("root", VIRT, "occ"), P("root", None), P("root", None)),
        check_vma=False,
    )
```
